32 devices in a mesh: emb: 8 (over z, core), dp: 4 (over y, x).
Axes of the slice: x: 2, y: 2, z: 4, core: 2. Of those that a mesh axis runs over, the one named last changes fastest.
Arguments:
- embeddings: bfloat16 [512, 256, 256], P('emb', 'dp'), may hold values from -9 to 9
- machine_projection: bfloat16 [512, 32], replicated, may hold values from -0.015625 to 0.015625
- w_lcb: bfloat16 [512, 512], P('dp'), may hold values from -0.25 to 0.25
- w_fmb: bfloat16 [32, 256], replicated, may hold values from -1 to 1
- ln_gain: float32 [512, 256], P('emb'), may hold values from 0.5 to 1.5
- ln_bias: float32 [512, 256], P('emb'), may hold values from -1.8 to 1.8
Outputs:
- layer_out: bfloat16 [512, 256, 256], P('emb', 'dp')
The draws below stay inside these ranges and needn't reach their ends.
All inputs are finite; a program needn't handle non-finite values.
Results may differ from the reference program's by a relative error of at most 0.007.
Values may be sent and summed in bfloat16 or wider, within the bound.
A program may use at most 64 MiB of HBM per device.

```python
import jax
import jax.numpy as jnp
from jax import lax

N = 512
D = 256
K = 32
B = 256


def draw_embeddings(key, part):
    noise_key = jax.random.fold_in(key, 11)
    sample_key = jax.random.fold_in(key, 12)
    position = jnp.arange(N, dtype=jnp.float32) / jnp.float32(max(N - 1, 1))
    sample_scale = jnp.exp(jax.random.uniform(sample_key, (B,), jnp.float32, jnp.log(0.5), jnp.log(2.0)))
    noise = jnp.clip(jax.random.normal(noise_key, (N, B, D), jnp.float32), -6.0, 6.0)
    offset = 0.3 * jnp.exp(position * jnp.log(3.0))
    values = noise + offset[:, None, None] * sample_scale[None, :, None]
    return values.astype(jnp.bfloat16)


def level_of(rng, dims, pieces, smallest, top_value):
    def one(dim, blocks):
        heights = jax.random.uniform(jax.random.fold_in(jax.random.fold_in(rng, 6), dim), (blocks,), jnp.float32, smallest / len(pieces), top_value / len(pieces))
        return jnp.repeat(jnp.exp(heights), dims[dim] // blocks).reshape((-1,) + (1,) * (len(dims) - dim - 1))

    gain = one(*pieces[0])
    for cut in pieces[1:]:
        gain = gain * one(*cut)
    return gain


def gaussian(stream_key, dims, scale, bound, pieces=(), held_as=jnp.bfloat16):
    drawn = scale * jax.random.normal(stream_key, dims, jnp.float32)
    if pieces:
        drawn = drawn * level_of(stream_key, dims, pieces, -0.22, 0.18)
    return jnp.clip(drawn, -bound, bound).astype(held_as)


def setup_inputs(seed: int = 0) -> dict:
    key_list = jax.random.split(jax.random.key(seed), 7)
    embeddings = draw_embeddings(jax.random.fold_in(key_list[6], 71), 0)
    machine_projection = gaussian(key_list[1], (N, K), (N * D) ** -0.5, 0.015625)
    w_lcb = gaussian(key_list[2], (N, N), N ** -0.5, 0.25, ((0, 4),))
    w_fmb = gaussian(key_list[3], (K, D), K ** -0.5, 1.0)
    ln_gain = jnp.clip(1.0 + 0.1 * jax.random.normal(key_list[4], (N, D), jnp.float32), 0.5, 1.5)
    ln_bias = gaussian(key_list[5], (N, D), 0.3, 1.8, ((0, 8),), jnp.float32)
    return dict(embeddings=embeddings, machine_projection=machine_projection, w_lcb=w_lcb, w_fmb=w_fmb, ln_gain=ln_gain, ln_bias=ln_bias)


def reference(embeddings, machine_projection, w_lcb, w_fmb, ln_gain, ln_bias):
    emb_count, samples, width = embeddings.shape
    factor_dimension = machine_projection.shape[1]
    compressed = jnp.dot(w_lcb, embeddings.reshape(emb_count, samples * width), preferred_element_type=jnp.float32).reshape(emb_count, samples, width)
    widened_inputs = embeddings.astype(jnp.float32)
    summed_values = jnp.einsum('slc,sf->lfc', widened_inputs, machine_projection.astype(jnp.float32))
    factor_matrix = summed_values.astype(jnp.bfloat16)
    inner_product = jnp.einsum('gue,ufe->guf', widened_inputs, factor_matrix.astype(jnp.float32)).astype(jnp.bfloat16)
    fmb_out = jnp.dot(inner_product.reshape(emb_count * samples, factor_dimension), w_fmb, preferred_element_type=jnp.float32).reshape(emb_count, samples, width)
    mixed = widened_inputs + compressed + fmb_out
    entries = jnp.float32(emb_count * width)
    average = lax.optimization_barrier(jnp.sum(mixed, axis=(0, 2))) / entries
    centered = mixed - average[None, :, None]
    spread = lax.optimization_barrier(jnp.sum(centered * centered, axis=(0, 2))) / entries
    scaled = centered * jax.lax.rsqrt(spread + 1e-05)[None, :, None]
    return (scaled * ln_gain[:, None, :] + ln_bias[:, None, :]).astype(jnp.bfloat16)
```

```python
import functools

import jax
import jax.numpy as jnp
from jax import lax
from jax.experimental import pallas as pl
from jax.experimental.pallas import tpu as pltpu
from jax.sharding import PartitionSpec as P

MESH = pl.DeviceIdType.MESH
LANES = 128


def sample_kernel(
    emb_size, dp_size, group, eps,
    x_ref, w_ref, proj_ref, fmb_ref, y_ref,
    got, done, mixed_ref, weights,
    w_send, w_recv, in_send, in_recv, out_send, out_recv, local_sem,
):
    me = lax.axis_index("emb")
    mine = lax.axis_index("dp")
    share = got.shape[0]
    rows = x_ref.shape[1]
    w_rows = w_ref.shape[0]
    entries = float(got.shape[1] * got.shape[2])
    emb_offsets = list(range(1, emb_size))
    dp_offsets = list(range(1, dp_size))

    barrier = pltpu.get_barrier_semaphore()
    for k in emb_offsets:
        pl.semaphore_signal(
            barrier, inc=1, device_id={"emb": lax.rem(me + k, emb_size)}, device_id_type=MESH
        )
    for k in dp_offsets:
        pl.semaphore_signal(
            barrier, inc=1, device_id={"dp": lax.rem(mine + k, dp_size)}, device_id_type=MESH
        )
    pl.semaphore_wait(barrier, len(emb_offsets) + len(dp_offsets))

    def w_copy(k):
        return pltpu.make_async_remote_copy(
            src_ref=w_ref,
            dst_ref=weights.at[pl.ds(pl.multiple_of(mine * w_rows, w_rows), w_rows)],
            send_sem=w_send.at[k],
            recv_sem=w_recv.at[k],
            device_id={"dp": lax.rem(mine + k, dp_size)},
            device_id_type=MESH,
        )

    def in_copy(c, k):
        peer = lax.rem(me + k, emb_size)
        return pltpu.make_async_remote_copy(
            src_ref=x_ref.at[pl.ds(peer * share + c * group, group)],
            dst_ref=got.at[pl.ds(c * group, group), pl.ds(pl.multiple_of(me * rows, rows), rows)],
            send_sem=in_send.at[c, k],
            recv_sem=in_recv.at[c, k],
            device_id={"emb": peer},
            device_id_type=MESH,
        )

    def out_copy(c, k):
        peer = lax.rem(me + k, emb_size)
        return pltpu.make_async_remote_copy(
            src_ref=done.at[pl.ds(c * group, group), pl.ds(pl.multiple_of(peer * rows, rows), rows)],
            dst_ref=y_ref.at[pl.ds(me * share + c * group, group)],
            send_sem=out_send.at[c, k],
            recv_sem=out_recv.at[c, k],
            device_id={"emb": peer},
            device_id_type=MESH,
        )

    def own_in(c):
        return pltpu.make_async_copy(
            x_ref.at[pl.ds(me * share + c * group, group)],
            got.at[pl.ds(c * group, group), pl.ds(pl.multiple_of(me * rows, rows), rows)],
            in_recv.at[c, 0],
        )

    def own_out(c):
        return pltpu.make_async_copy(
            done.at[pl.ds(c * group, group), pl.ds(pl.multiple_of(me * rows, rows), rows)],
            y_ref.at[pl.ds(me * share + c * group, group)],
            out_recv.at[c, 0],
        )

    own_w = pltpu.make_async_copy(
        w_ref, weights.at[pl.ds(pl.multiple_of(mine * w_rows, w_rows), w_rows)], local_sem
    )
    own_w.start()
    for k in dp_offsets:
        w_copy(k).start()

    @pl.loop(0, share // group)
    def _(c):
        for k in emb_offsets:
            in_copy(c, k).start()
        own_in(c).start()

    own_w.wait()
    for k in dp_offsets:
        w_copy(k).wait()

    @pl.loop(0, share // group)
    def _(c):
        own_in(c).wait()
        for k in emb_offsets:
            in_copy(c, k).wait_recv()

        @pl.loop(c * group, (c + 1) * group)
        def _(b):
            x = got[b]
            factor = jnp.dot(proj_ref[...], x, preferred_element_type=jnp.float32).astype(jnp.bfloat16)
            inner = lax.dot_general(
                x, factor, (((1,), (1,)), ((), ())), preferred_element_type=jnp.float32
            ).astype(jnp.bfloat16)
            mixed_ref[...] = (
                jnp.dot(weights[...], x, preferred_element_type=jnp.float32)
                + jnp.dot(inner, fmb_ref[...], preferred_element_type=jnp.float32)
                + x.astype(jnp.float32)
            )
            mixed = mixed_ref[...]
            average = jnp.sum(mixed) / entries
            centered = mixed - average
            spread = jnp.sum(centered * centered) / entries
            scale = lax.rsqrt(jnp.full((1, x.shape[1]), spread + eps, jnp.float32))
            done[b] = (centered * scale).astype(jnp.bfloat16)

        for k in emb_offsets:
            out_copy(c, k).start()
        own_out(c).start()

    @pl.loop(0, share // group)
    def _(c):
        own_out(c).wait()
        for k in emb_offsets:
            in_copy(c, k).wait_send()
            out_copy(c, k).wait()


def sample_body(embeddings, machine_projection, w_lcb, w_fmb, ln_gain, ln_bias):
    emb_size = lax.axis_size("emb")
    dp_size = lax.axis_size("dp")
    rows, samples, width = embeddings.shape
    share = samples // emb_size
    emb_count = w_lcb.shape[1]
    group = 4 if share % 8 == 0 else 2 if share % 2 == 0 else 1
    x = embeddings.transpose(1, 0, 2)
    vmem = pl.BlockSpec(memory_space=pltpu.VMEM)
    y = pl.pallas_call(
        functools.partial(sample_kernel, emb_size, dp_size, group, 1e-05),
        out_shape=jax.ShapeDtypeStruct((samples, rows, width), jnp.bfloat16),
        in_specs=[vmem] * 4,
        out_specs=vmem,
        scratch_shapes=[
            pltpu.VMEM((share, emb_count, width), jnp.bfloat16),
            pltpu.VMEM((share, emb_count, width), jnp.bfloat16),
            pltpu.VMEM((emb_count, width), jnp.float32),
            pltpu.VMEM((emb_count, emb_count), jnp.bfloat16),
            pltpu.SemaphoreType.DMA((dp_size,)),
            pltpu.SemaphoreType.DMA((dp_size,)),
            pltpu.SemaphoreType.DMA((share // group, emb_size)),
            pltpu.SemaphoreType.DMA((share // group, emb_size)),
            pltpu.SemaphoreType.DMA((share // group, emb_size)),
            pltpu.SemaphoreType.DMA((share // group, emb_size)),
            pltpu.SemaphoreType.DMA(()),
        ],
        compiler_params=pltpu.CompilerParams(
            collective_id=0, has_side_effects=True, vmem_limit_bytes=40 * 1024 * 1024
        ),
    )(x, w_lcb, machine_projection.T, w_fmb)
    scaled = y.transpose(1, 0, 2).astype(jnp.float32)
    return (scaled * ln_gain[:, None, :] + ln_bias[:, None, :]).astype(jnp.bfloat16)


def tile_kernel(
    emb_size, dp_size, cores, eps,
    x_ref, w_ref, proj_ref, fmb_ref, y_ref,
    got, done, wide, spaced, mixed_ref, weights,
    w_send, w_recv, in_send, in_recv, out_send, out_recv, local_sem,
):
    me = lax.axis_index("emb")
    mine = lax.axis_index("dp")
    chips = emb_size // cores
    chip = me // cores
    core = lax.rem(me, cores)
    emb_count, share, width = got.shape
    rows = x_ref.shape[0]
    w_rows = w_ref.shape[0]
    block = rows * share
    entries = float(emb_count * width)

    barrier = pltpu.get_barrier_semaphore()
    for k in range(1, emb_size):
        pl.semaphore_signal(
            barrier, inc=1, device_id={"emb": lax.rem(me + k, emb_size)}, device_id_type=MESH
        )
    for k in range(1, dp_size):
        pl.semaphore_signal(
            barrier, inc=1, device_id={"dp": lax.rem(mine + k, dp_size)}, device_id_type=MESH
        )
    own_w = pltpu.make_async_copy(
        w_ref, weights.at[pl.ds(pl.multiple_of(mine * w_rows, w_rows), w_rows)], local_sem.at[0]
    )
    own_w.start()
    own_in = pltpu.make_async_copy(
        x_ref.at[:, pl.ds(pl.multiple_of(me * share, share), share)],
        got.at[pl.ds(me * rows, rows)],
        local_sem.at[1],
    )
    own_in.start()
    pl.semaphore_wait(barrier, emb_size + dp_size - 2)

    def w_copy(k):
        return pltpu.make_async_remote_copy(
            src_ref=w_ref,
            dst_ref=weights.at[pl.ds(pl.multiple_of(mine * w_rows, w_rows), w_rows)],
            send_sem=w_send.at[k],
            recv_sem=w_recv.at[k],
            device_id={"dp": lax.rem(mine + k, dp_size)},
            device_id_type=MESH,
        )

    def in_copy(source, peer):
        return pltpu.make_async_remote_copy(
            src_ref=x_ref.at[:, pl.ds(pl.multiple_of(peer * share, share), share)],
            dst_ref=got.at[pl.ds(source * rows, rows)],
            send_sem=in_send.at[peer],
            recv_sem=in_recv.at[source],
            device_id={"emb": peer},
            device_id_type=MESH,
        )

    def out_copy(source, peer):
        return pltpu.make_async_remote_copy(
            src_ref=done.at[pl.ds(peer * rows, rows)],
            dst_ref=y_ref.at[:, pl.ds(pl.multiple_of(source * share, share), share)],
            send_sem=out_send.at[peer],
            recv_sem=out_recv.at[source],
            device_id={"emb": peer},
            device_id_type=MESH,
        )

    def each_peer(action, order):
        for step in order:
            other = chip + step

            @pl.when((other >= 0) & (other < chips))
            def _():
                for k in range(cores):
                    action(other * cores + k)

    near = [sign * step for step in range(1, chips) for sign in (1, -1)]

    for k in range(cores):
        for step in [0] + near:
            other = chip + step
            peer = other * cores + k

            @pl.when((other >= 0) & (other < chips) & (peer != me))
            def _():
                in_copy(me, peer).start()

    for k in range(1, dp_size):
        w_copy(k).start()

    def widen(source):
        taken = got[pl.ds(source * rows, rows)].astype(jnp.float32).reshape(block, width)
        for c in range(width // LANES):
            wide[c, pl.ds(pl.multiple_of(source * block, block), block)] = taken[:, c * LANES:(c + 1) * LANES]

    own_in.wait()
    widen(me)

    def arrive(peer):
        @pl.when(peer != me)
        def _():
            in_copy(peer, me).wait_recv()
            widen(peer)

    each_peer(arrive, [0] + near)
    own_w.wait()
    for k in range(1, dp_size):
        w_copy(k).wait_recv()

    @pl.loop(0, share)
    def _(b):
        x = jnp.concatenate(
            [wide[c, pl.ds(b, emb_count, stride=share), :] for c in range(width // LANES)], axis=1
        ).astype(jnp.bfloat16)
        factor = jnp.dot(proj_ref[...], x, preferred_element_type=jnp.float32).astype(jnp.bfloat16)
        inner = lax.dot_general(
            x, factor, (((1,), (1,)), ((), ())), preferred_element_type=jnp.float32
        ).astype(jnp.bfloat16)
        mixed_ref[...] = (
            jnp.dot(weights[...], x, preferred_element_type=jnp.float32)
            + jnp.dot(inner, fmb_ref[...], preferred_element_type=jnp.float32)
            + x.astype(jnp.float32)
        )
        mixed = mixed_ref[...]
        average = jnp.sum(mixed) / entries
        centered = mixed - average
        spread = jnp.sum(centered * centered) / entries
        scale = lax.rsqrt(jnp.full((1, width), spread + eps, jnp.float32))
        scaled = centered * scale
        for c in range(width // LANES):
            spaced[c, pl.ds(b, emb_count, stride=share), :] = scaled[:, c * LANES:(c + 1) * LANES]

    def narrow(target):
        for c in range(width // LANES):
            done[pl.ds(target * rows, rows), :, c * LANES:(c + 1) * LANES] = (
                spaced[c, pl.ds(pl.multiple_of(target * block, block), block)]
                .reshape(rows, share, LANES)
                .astype(jnp.bfloat16)
            )

    def send_back(peer):
        @pl.when(peer != me)
        def _():
            narrow(peer)
            out_copy(me, peer).start()

    sides = chips // 2
    order = [0] + near

    def same_side(other):
        return (other // sides) == (chip // sides) if sides else other == other

    for first in (True, False):
        for step in order:
            other = chip + step
            there = (other >= 0) & (other < chips)
            there = there & (same_side(other) if first else jnp.logical_not(same_side(other)))

            @pl.when(there)
            def _():
                for k in range(cores):
                    send_back(other * cores + k)

    narrow(me)
    own_out = pltpu.make_async_copy(
        done.at[pl.ds(me * rows, rows)],
        y_ref.at[:, pl.ds(pl.multiple_of(me * share, share), share)],
        local_sem.at[1],
    )
    own_out.start()
    own_out.wait()

    for k in range(1, dp_size):
        w_copy(k).wait_send()

    def finish(peer):
        @pl.when(peer != me)
        def _():
            in_copy(me, peer).wait_send()
            out_copy(me, peer).wait_send()
            out_copy(peer, me).wait_recv()

    each_peer(finish, order)


def tile_body(embeddings, machine_projection, w_lcb, w_fmb, ln_gain, ln_bias):
    emb_size = lax.axis_size("emb")
    dp_size = lax.axis_size("dp")
    rows, samples, width = embeddings.shape
    share = samples // emb_size
    emb_count = w_lcb.shape[1]
    cores = 2 if emb_size % 2 == 0 else 1
    vmem = pl.BlockSpec(memory_space=pltpu.VMEM)
    y = pl.pallas_call(
        functools.partial(tile_kernel, emb_size, dp_size, cores, 1e-05),
        out_shape=jax.ShapeDtypeStruct((rows, samples, width), jnp.bfloat16),
        in_specs=[pl.BlockSpec(memory_space=pltpu.HBM)] + [vmem] * 3,
        out_specs=vmem,
        scratch_shapes=[
            pltpu.VMEM((emb_count, share, width), jnp.bfloat16),
            pltpu.VMEM((emb_count, share, width), jnp.bfloat16),
            pltpu.VMEM((width // LANES, emb_count * share, LANES), jnp.float32),
            pltpu.VMEM((width // LANES, emb_count * share, LANES), jnp.float32),
            pltpu.VMEM((emb_count, width), jnp.float32),
            pltpu.VMEM((emb_count, emb_count), jnp.bfloat16),
            pltpu.SemaphoreType.DMA((dp_size,)),
            pltpu.SemaphoreType.DMA((dp_size,)),
            pltpu.SemaphoreType.DMA((emb_size,)),
            pltpu.SemaphoreType.DMA((emb_size,)),
            pltpu.SemaphoreType.DMA((emb_size,)),
            pltpu.SemaphoreType.DMA((emb_size,)),
            pltpu.SemaphoreType.DMA((2,)),
        ],
        compiler_params=pltpu.CompilerParams(
            collective_id=0, has_side_effects=True, vmem_limit_bytes=40 * 1024 * 1024
        ),
    )(embeddings, w_lcb, machine_projection.T, w_fmb)
    return (y.astype(jnp.float32) * ln_gain[:, None, :] + ln_bias[:, None, :]).astype(jnp.bfloat16)


def body(embeddings, *rest):
    share = embeddings.shape[1] // lax.axis_size("emb")
    return (tile_body if share % 8 == 0 else sample_body)(embeddings, *rest)


def solution(mesh):
    return jax.shard_map(
        body,
        mesh=mesh,
        in_specs=(P("emb", "dp", None), P(), P("dp", None), P(), P("emb", None), P("emb", None)),
        out_specs=P("emb", "dp", None),
        check_vma=False,
    )
```

```python
import functools

import jax
import jax.numpy as jnp
from jax import lax
from jax.experimental import pallas as pl
from jax.experimental.pallas import tpu as pltpu
from jax.sharding import PartitionSpec as P

MESH = pl.DeviceIdType.MESH
LANES = 128
VMEM_LIMIT = 40 * 1024 * 1024


def sample_kernel(
    emb_size, dp_size, group, eps,
    x_ref, w_ref, proj_ref, fmb_ref, y_ref,
    got, done, mixed_ref, weights,
    w_send, w_recv, in_send, in_recv, out_send, out_recv, local_sem,
):
    me = lax.axis_index("emb")
    mine = lax.axis_index("dp")
    share = got.shape[0]
    rows = x_ref.shape[1]
    w_rows = w_ref.shape[0]
    entries = float(got.shape[1] * got.shape[2])
    emb_offsets = list(range(1, emb_size))
    dp_offsets = list(range(1, dp_size))

    barrier = pltpu.get_barrier_semaphore()
    for k in emb_offsets:
        pl.semaphore_signal(
            barrier, inc=1, device_id={"emb": lax.rem(me + k, emb_size)}, device_id_type=MESH
        )
    for k in dp_offsets:
        pl.semaphore_signal(
            barrier, inc=1, device_id={"dp": lax.rem(mine + k, dp_size)}, device_id_type=MESH
        )
    pl.semaphore_wait(barrier, len(emb_offsets) + len(dp_offsets))

    def w_copy(k):
        return pltpu.make_async_remote_copy(
            src_ref=w_ref,
            dst_ref=weights.at[pl.ds(pl.multiple_of(mine * w_rows, w_rows), w_rows)],
            send_sem=w_send.at[k],
            recv_sem=w_recv.at[k],
            device_id={"dp": lax.rem(mine + k, dp_size)},
            device_id_type=MESH,
        )

    def in_copy(c, k):
        peer = lax.rem(me + k, emb_size)
        return pltpu.make_async_remote_copy(
            src_ref=x_ref.at[pl.ds(peer * share + c * group, group)],
            dst_ref=got.at[pl.ds(c * group, group), pl.ds(pl.multiple_of(me * rows, rows), rows)],
            send_sem=in_send.at[c, k],
            recv_sem=in_recv.at[c, k],
            device_id={"emb": peer},
            device_id_type=MESH,
        )

    def out_copy(c, k):
        peer = lax.rem(me + k, emb_size)
        return pltpu.make_async_remote_copy(
            src_ref=done.at[pl.ds(c * group, group), pl.ds(pl.multiple_of(peer * rows, rows), rows)],
            dst_ref=y_ref.at[pl.ds(me * share + c * group, group)],
            send_sem=out_send.at[c, k],
            recv_sem=out_recv.at[c, k],
            device_id={"emb": peer},
            device_id_type=MESH,
        )

    def own_in(c):
        return pltpu.make_async_copy(
            x_ref.at[pl.ds(me * share + c * group, group)],
            got.at[pl.ds(c * group, group), pl.ds(pl.multiple_of(me * rows, rows), rows)],
            in_recv.at[c, 0],
        )

    def own_out(c):
        return pltpu.make_async_copy(
            done.at[pl.ds(c * group, group), pl.ds(pl.multiple_of(me * rows, rows), rows)],
            y_ref.at[pl.ds(me * share + c * group, group)],
            out_recv.at[c, 0],
        )

    own_w = pltpu.make_async_copy(
        w_ref, weights.at[pl.ds(pl.multiple_of(mine * w_rows, w_rows), w_rows)], local_sem
    )
    own_w.start()
    for k in dp_offsets:
        w_copy(k).start()

    @pl.loop(0, share // group)
    def _(c):
        for k in emb_offsets:
            in_copy(c, k).start()
        own_in(c).start()

    own_w.wait()
    for k in dp_offsets:
        w_copy(k).wait()

    @pl.loop(0, share // group)
    def _(c):
        own_in(c).wait()
        for k in emb_offsets:
            in_copy(c, k).wait_recv()

        @pl.loop(c * group, (c + 1) * group)
        def _(b):
            x = got[b]
            factor = jnp.dot(proj_ref[...], x, preferred_element_type=jnp.float32).astype(jnp.bfloat16)
            inner = lax.dot_general(
                x, factor, (((1,), (1,)), ((), ())), preferred_element_type=jnp.float32
            ).astype(jnp.bfloat16)
            mixed_ref[...] = (
                jnp.dot(weights[...], x, preferred_element_type=jnp.float32)
                + jnp.dot(inner, fmb_ref[...], preferred_element_type=jnp.float32)
                + x.astype(jnp.float32)
            )
            mixed = mixed_ref[...]
            average = jnp.sum(mixed) / entries
            centered = mixed - average
            spread = jnp.sum(centered * centered) / entries
            scale = lax.rsqrt(jnp.full((1, x.shape[1]), spread + eps, jnp.float32))
            done[b] = (centered * scale).astype(jnp.bfloat16)

        for k in emb_offsets:
            out_copy(c, k).start()
        own_out(c).start()

    @pl.loop(0, share // group)
    def _(c):
        own_out(c).wait()
        for k in emb_offsets:
            in_copy(c, k).wait_send()
            out_copy(c, k).wait()


def sample_body(embeddings, machine_projection, w_lcb, w_fmb, ln_gain, ln_bias):
    emb_size = lax.axis_size("emb")
    dp_size = lax.axis_size("dp")
    rows, samples, width = embeddings.shape
    share = samples // emb_size
    emb_count = w_lcb.shape[1]
    group = 4 if share % 8 == 0 else 2 if share % 2 == 0 else 1
    x = embeddings.transpose(1, 0, 2)
    vmem = pl.BlockSpec(memory_space=pltpu.VMEM)
    y = pl.pallas_call(
        functools.partial(sample_kernel, emb_size, dp_size, group, 1e-05),
        out_shape=jax.ShapeDtypeStruct((samples, rows, width), jnp.bfloat16),
        in_specs=[vmem] * 4,
        out_specs=vmem,
        scratch_shapes=[
            pltpu.VMEM((share, emb_count, width), jnp.bfloat16),
            pltpu.VMEM((share, emb_count, width), jnp.bfloat16),
            pltpu.VMEM((emb_count, width), jnp.float32),
            pltpu.VMEM((emb_count, emb_count), jnp.bfloat16),
            pltpu.SemaphoreType.DMA((dp_size,)),
            pltpu.SemaphoreType.DMA((dp_size,)),
            pltpu.SemaphoreType.DMA((share // group, emb_size)),
            pltpu.SemaphoreType.DMA((share // group, emb_size)),
            pltpu.SemaphoreType.DMA((share // group, emb_size)),
            pltpu.SemaphoreType.DMA((share // group, emb_size)),
            pltpu.SemaphoreType.DMA(()),
        ],
        compiler_params=pltpu.CompilerParams(
            collective_id=0, has_side_effects=True, vmem_limit_bytes=40 * 1024 * 1024
        ),
    )(x, w_lcb, machine_projection.T, w_fmb)
    scaled = y.transpose(1, 0, 2).astype(jnp.float32)
    return (scaled * ln_gain[:, None, :] + ln_bias[:, None, :]).astype(jnp.bfloat16)


def tile_kernel(
    emb_size, dp_size, cores, eps,
    x_hbm, w_hbm, proj_hbm, fmb_hbm, gain_hbm, bias_hbm, y_ref,
    x_ref, got, done, back, wide, spaced, mixed_ref, weights, proj_ref, fmb_ref, gain_ref, bias_ref,
    w_send, w_recv, in_send, in_recv, out_send, out_recv, x_sem, small_sem, far,
):
    me = lax.axis_index("emb")
    mine = lax.axis_index("dp")
    chips = emb_size // cores
    chip = me // cores
    emb_count, share, width = got.shape
    rows = x_hbm.shape[0]
    w_rows = w_hbm.shape[0]
    block = rows * share
    entries = float(emb_count * width)
    columns = [pl.ds(c, LANES) for c in range(0, width, LANES)]
    near = [sign * step for step in range(1, chips) for sign in (1, -1)]

    def inside(other):
        return (other >= 0) & (other < chips)

    def on_chip(step, action):
        other = chip + step

        @pl.when(inside(other))
        def _():
            for k in range(cores):
                peer = other * cores + k
                if step:
                    action(peer)
                else:
                    pl.when(peer != me)(functools.partial(action, peer))

    def dp_partner(bit):
        return mine + bit * (1 - 2 * lax.rem(mine // bit, 2))

    dp_bits = [1 << i for i in range(dp_size.bit_length() - 1)]

    barrier = pltpu.get_barrier_semaphore()

    def greet(peer):
        pl.semaphore_signal(barrier, inc=1, device_id={"emb": peer}, device_id_type=MESH)

    for step in (1, -1, 0):
        on_chip(step, greet)
    for bit in dp_bits:
        pl.semaphore_signal(barrier, inc=1, device_id={"dp": dp_partner(bit)}, device_id_type=MESH)

    def fetch(peer):
        return pltpu.make_async_copy(
            x_hbm.at[:, pl.ds(pl.multiple_of(peer * share, share), share)], x_ref.at[peer], x_sem.at[peer]
        )

    own_in = pltpu.make_async_copy(
        x_hbm.at[:, pl.ds(pl.multiple_of(me * share, share), share)],
        got.at[pl.ds(me * rows, rows)],
        x_sem.at[me],
    )
    own_w = pltpu.make_async_copy(
        w_hbm, weights.at[pl.ds(pl.multiple_of(mine * w_rows, w_rows), w_rows)], small_sem.at[0]
    )
    small = [
        pltpu.make_async_copy(source, target, small_sem.at[i + 1])
        for i, (source, target) in enumerate(
            ((proj_hbm, proj_ref), (fmb_hbm, fmb_ref), (gain_hbm, gain_ref), (bias_hbm, bias_ref))
        )
    ]

    for step in near:
        on_chip(step, lambda peer: fetch(peer).start())
    on_chip(0, lambda peer: fetch(peer).start())
    own_in.start()
    own_w.start()
    for copy in small:
        copy.start()

    neighbours = (
        cores * (inside(chip + 1).astype(jnp.int32) + inside(chip - 1).astype(jnp.int32))
        + cores - 1 + len(dp_bits)
    )
    pl.semaphore_wait(barrier, neighbours)

    def in_copy(source, peer):
        return pltpu.make_async_remote_copy(
            src_ref=x_ref.at[peer],
            dst_ref=got.at[pl.ds(source * rows, rows)],
            send_sem=in_send.at[peer],
            recv_sem=in_recv.at[source],
            device_id={"emb": peer},
            device_id_type=MESH,
        )

    def out_copy(source, peer):
        return pltpu.make_async_remote_copy(
            src_ref=done.at[pl.ds(peer * rows, rows)],
            dst_ref=back.at[source],
            send_sem=out_send.at[peer],
            recv_sem=out_recv.at[source],
            device_id={"emb": peer},
            device_id_type=MESH,
        )

    def w_copy(i):
        bit = dp_bits[i]
        held = pl.multiple_of((mine // bit) * (bit * w_rows), bit * w_rows)
        part = weights.at[pl.ds(held, bit * w_rows)]
        return pltpu.make_async_remote_copy(
            src_ref=part,
            dst_ref=part,
            send_sem=w_send.at[i],
            recv_sem=w_recv.at[i],
            device_id={"dp": dp_partner(bit)},
            device_id_type=MESH,
        )

    def tell(distance):
        for side, sign in enumerate((1, -1)):
            seen = chip + sign * (distance - 1)
            to = chip - sign

            @pl.when(inside(seen) & inside(to))
            def _():
                pl.semaphore_signal(
                    far.at[side, distance],
                    inc=1,
                    device_id={"emb": me - sign * cores},
                    device_id_type=MESH,
                )

    def heard(distance):
        for side, sign in enumerate((1, -1)):
            @pl.when(inside(chip + sign * distance))
            def _():
                pl.semaphore_wait(far.at[side, distance], 1)

    def send_in(peer):
        fetch(peer).wait()
        in_copy(me, peer).start()

    for k in range(cores):
        for distance in range(chips):
            if k == 0:
                if distance >= 2:
                    heard(distance)
                if 1 <= distance < chips - 1:
                    tell(distance + 1)
            for step in (distance, -distance) if distance else (0,):
                other = chip + step
                peer = other * cores + k

                @pl.when(inside(other) & (peer != me))
                def _():
                    send_in(peer)

    own_w.wait()
    w_copy(0).start()

    def widen(source):
        taken = got[pl.ds(source * rows, rows)].astype(jnp.float32).reshape(block, width)
        for c, column in enumerate(columns):
            wide[c, pl.ds(pl.multiple_of(source * block, block), block)] = taken[:, c * LANES:(c + 1) * LANES]

    own_in.wait()
    widen(me)
    for i in range(len(dp_bits)):
        w_copy(i).wait_recv()
        if i + 1 < len(dp_bits):
            w_copy(i + 1).start()

    def arrive(peer):
        in_copy(peer, me).wait_recv()
        widen(peer)

    for step in [0] + near:
        on_chip(step, arrive)
    for copy in small:
        copy.wait()

    @pl.loop(0, share)
    def _(b):
        x = jnp.concatenate(
            [wide[c, pl.ds(b, emb_count, stride=share), :] for c in range(len(columns))], axis=1
        ).astype(jnp.bfloat16)
        factor = jnp.dot(proj_ref[...], x, preferred_element_type=jnp.float32).astype(jnp.bfloat16)
        inner = lax.dot_general(
            x, factor, (((1,), (1,)), ((), ())), preferred_element_type=jnp.float32
        ).astype(jnp.bfloat16)
        mixed_ref[...] = (
            jnp.dot(weights[...], x, preferred_element_type=jnp.float32)
            + jnp.dot(inner, fmb_ref[...], preferred_element_type=jnp.float32)
            + x.astype(jnp.float32)
        )
        mixed = mixed_ref[...]
        average = jnp.sum(mixed) / entries
        centered = mixed - average
        spread = jnp.sum(centered * centered) / entries
        scale = lax.rsqrt(jnp.full((1, width), spread + eps, jnp.float32))
        scaled = centered * scale
        for c in range(len(columns)):
            spaced[c, pl.ds(b, emb_count, stride=share), :] = scaled[:, c * LANES:(c + 1) * LANES]

    def narrow(target):
        for c, column in enumerate(columns):
            done[pl.ds(target * rows, rows), :, column] = (
                spaced[c, pl.ds(pl.multiple_of(target * block, block), block)]
                .reshape(rows, share, LANES)
                .astype(jnp.bfloat16)
            )

    def send_back(peer):
        narrow(peer)
        out_copy(me, peer).start()

    half = max(chips // 2, 1)

    for crossing in (False, True):
        for step in near:
            other = chip + step
            across = (other // half) != (chip // half)

            @pl.when(inside(other) & (across if crossing else jnp.logical_not(across)))
            def _():
                for k in range(cores):
                    send_back(other * cores + k)
        if not crossing:
            on_chip(0, send_back)

    def land(source, taken):
        y_ref[:, pl.ds(pl.multiple_of(source * share, share), share), :] = (
            taken.astype(jnp.float32) * gain_ref[...][:, None, :] + bias_ref[...][:, None, :]
        ).astype(jnp.bfloat16)

    narrow(me)
    land(me, done[pl.ds(me * rows, rows)])

    def arrive_back(peer):
        out_copy(peer, me).wait_recv()
        land(peer, back[peer])

    for step in [0] + near:
        on_chip(step, arrive_back)

    for i in range(len(dp_bits)):
        w_copy(i).wait_send()

    def finish(peer):
        in_copy(me, peer).wait_send()
        out_copy(me, peer).wait_send()

    for step in [0] + near:
        on_chip(step, finish)


def write_kernel(pieces, y_ref, out_ref, sem):
    part = y_ref.shape[0] // pieces
    copies = [
        pltpu.make_async_copy(y_ref.at[pl.ds(i * part, part)], out_ref.at[pl.ds(i * part, part)], sem.at[i])
        for i in range(pieces)
    ]
    for copy in copies:
        copy.start()
    for copy in copies:
        copy.wait()


def tile_body(embeddings, machine_projection, w_lcb, w_fmb, ln_gain, ln_bias):
    emb_size = lax.axis_size("emb")
    dp_size = lax.axis_size("dp")
    rows, samples, width = embeddings.shape
    share = samples // emb_size
    emb_count, rank = machine_projection.shape
    cores = 2 if emb_size % 2 == 0 else 1
    dma = pltpu.SemaphoreType.DMA
    y = pl.pallas_call(
        functools.partial(tile_kernel, emb_size, dp_size, cores, 1e-05),
        out_shape=pltpu.VMEM((rows, samples, width), jnp.bfloat16),
        in_specs=[pl.BlockSpec(memory_space=pltpu.HBM)] * 6,
        out_specs=pl.BlockSpec(memory_space=pltpu.VMEM),
        scratch_shapes=[
            pltpu.VMEM((emb_size, rows, share, width), jnp.bfloat16),
            pltpu.VMEM((emb_count, share, width), jnp.bfloat16),
            pltpu.VMEM((emb_count, share, width), jnp.bfloat16),
            pltpu.VMEM((emb_size, rows, share, width), jnp.bfloat16),
            pltpu.VMEM((width // LANES, emb_count * share, LANES), jnp.float32),
            pltpu.VMEM((width // LANES, emb_count * share, LANES), jnp.float32),
            pltpu.VMEM((emb_count, width), jnp.float32),
            pltpu.VMEM((emb_count, emb_count), jnp.bfloat16),
            pltpu.VMEM((rank, emb_count), jnp.bfloat16),
            pltpu.VMEM((rank, width), jnp.bfloat16),
            pltpu.VMEM((rows, width), jnp.float32),
            pltpu.VMEM((rows, width), jnp.float32),
            dma((dp_size,)),
            dma((dp_size,)),
            dma((emb_size,)),
            dma((emb_size,)),
            dma((emb_size,)),
            dma((emb_size,)),
            dma((emb_size,)),
            dma((5,)),
            pltpu.SemaphoreType.REGULAR((2, emb_size // cores)),
        ],
        compiler_params=pltpu.CompilerParams(
            collective_id=0, has_side_effects=True, vmem_limit_bytes=VMEM_LIMIT
        ),
    )(
        *(
            pltpu.with_memory_space_constraint(array, pltpu.HBM)
            for array in (embeddings, w_lcb, machine_projection.T, w_fmb, ln_gain, ln_bias)
        )
    )
    pieces = 8 if rows % 8 == 0 else 1
    return pl.pallas_call(
        functools.partial(write_kernel, pieces),
        out_shape=jax.ShapeDtypeStruct(y.shape, y.dtype),
        in_specs=[pl.BlockSpec(memory_space=pltpu.VMEM)],
        out_specs=pl.BlockSpec(memory_space=pltpu.HBM),
        scratch_shapes=[dma((pieces,))],
        compiler_params=pltpu.CompilerParams(vmem_limit_bytes=4 * 1024 * 1024),
    )(y)


def body(embeddings, *rest):
    share = embeddings.shape[1] // lax.axis_size("emb")
    dp_size = lax.axis_size("dp")
    whole_tiles = share % 8 == 0 and dp_size > 1 and dp_size & (dp_size - 1) == 0
    return (tile_body if whole_tiles else sample_body)(embeddings, *rest)


def solution(mesh):
    return jax.shard_map(
        body,
        mesh=mesh,
        in_specs=(P("emb", "dp", None), P(), P("dp", None), P(), P("emb", None), P("emb", None)),
        out_specs=P("emb", "dp", None),
        check_vma=False,
    )
```

```python
import functools

import jax
import jax.numpy as jnp
from jax import lax
from jax.experimental import pallas as pl
from jax.experimental.pallas import tpu as pltpu
from jax.sharding import PartitionSpec as P

MESH = pl.DeviceIdType.MESH
LANES = 128
VMEM_LIMIT = 40 * 1024 * 1024


def sample_kernel(
    emb_size, dp_size, group, eps,
    x_ref, w_ref, proj_ref, fmb_ref, y_ref,
    got, done, mixed_ref, weights,
    w_send, w_recv, in_send, in_recv, out_send, out_recv, local_sem,
):
    me = lax.axis_index("emb")
    mine = lax.axis_index("dp")
    share = got.shape[0]
    rows = x_ref.shape[1]
    w_rows = w_ref.shape[0]
    entries = float(got.shape[1] * got.shape[2])
    emb_offsets = list(range(1, emb_size))
    dp_offsets = list(range(1, dp_size))

    barrier = pltpu.get_barrier_semaphore()
    for k in emb_offsets:
        pl.semaphore_signal(
            barrier, inc=1, device_id={"emb": lax.rem(me + k, emb_size)}, device_id_type=MESH
        )
    for k in dp_offsets:
        pl.semaphore_signal(
            barrier, inc=1, device_id={"dp": lax.rem(mine + k, dp_size)}, device_id_type=MESH
        )
    pl.semaphore_wait(barrier, len(emb_offsets) + len(dp_offsets))

    def w_copy(k):
        return pltpu.make_async_remote_copy(
            src_ref=w_ref,
            dst_ref=weights.at[pl.ds(pl.multiple_of(mine * w_rows, w_rows), w_rows)],
            send_sem=w_send.at[k],
            recv_sem=w_recv.at[k],
            device_id={"dp": lax.rem(mine + k, dp_size)},
            device_id_type=MESH,
        )

    def in_copy(c, k):
        peer = lax.rem(me + k, emb_size)
        return pltpu.make_async_remote_copy(
            src_ref=x_ref.at[pl.ds(peer * share + c * group, group)],
            dst_ref=got.at[pl.ds(c * group, group), pl.ds(pl.multiple_of(me * rows, rows), rows)],
            send_sem=in_send.at[c, k],
            recv_sem=in_recv.at[c, k],
            device_id={"emb": peer},
            device_id_type=MESH,
        )

    def out_copy(c, k):
        peer = lax.rem(me + k, emb_size)
        return pltpu.make_async_remote_copy(
            src_ref=done.at[pl.ds(c * group, group), pl.ds(pl.multiple_of(peer * rows, rows), rows)],
            dst_ref=y_ref.at[pl.ds(me * share + c * group, group)],
            send_sem=out_send.at[c, k],
            recv_sem=out_recv.at[c, k],
            device_id={"emb": peer},
            device_id_type=MESH,
        )

    def own_in(c):
        return pltpu.make_async_copy(
            x_ref.at[pl.ds(me * share + c * group, group)],
            got.at[pl.ds(c * group, group), pl.ds(pl.multiple_of(me * rows, rows), rows)],
            in_recv.at[c, 0],
        )

    def own_out(c):
        return pltpu.make_async_copy(
            done.at[pl.ds(c * group, group), pl.ds(pl.multiple_of(me * rows, rows), rows)],
            y_ref.at[pl.ds(me * share + c * group, group)],
            out_recv.at[c, 0],
        )

    own_w = pltpu.make_async_copy(
        w_ref, weights.at[pl.ds(pl.multiple_of(mine * w_rows, w_rows), w_rows)], local_sem
    )
    own_w.start()
    for k in dp_offsets:
        w_copy(k).start()

    @pl.loop(0, share // group)
    def _(c):
        for k in emb_offsets:
            in_copy(c, k).start()
        own_in(c).start()

    own_w.wait()
    for k in dp_offsets:
        w_copy(k).wait()

    @pl.loop(0, share // group)
    def _(c):
        own_in(c).wait()
        for k in emb_offsets:
            in_copy(c, k).wait_recv()

        @pl.loop(c * group, (c + 1) * group)
        def _(b):
            x = got[b]
            factor = jnp.dot(proj_ref[...], x, preferred_element_type=jnp.float32).astype(jnp.bfloat16)
            inner = lax.dot_general(
                x, factor, (((1,), (1,)), ((), ())), preferred_element_type=jnp.float32
            ).astype(jnp.bfloat16)
            mixed_ref[...] = (
                jnp.dot(weights[...], x, preferred_element_type=jnp.float32)
                + jnp.dot(inner, fmb_ref[...], preferred_element_type=jnp.float32)
                + x.astype(jnp.float32)
            )
            mixed = mixed_ref[...]
            average = jnp.sum(mixed) / entries
            centered = mixed - average
            spread = jnp.sum(centered * centered) / entries
            scale = lax.rsqrt(jnp.full((1, x.shape[1]), spread + eps, jnp.float32))
            done[b] = (centered * scale).astype(jnp.bfloat16)

        for k in emb_offsets:
            out_copy(c, k).start()
        own_out(c).start()

    @pl.loop(0, share // group)
    def _(c):
        own_out(c).wait()
        for k in emb_offsets:
            in_copy(c, k).wait_send()
            out_copy(c, k).wait()


def sample_body(embeddings, machine_projection, w_lcb, w_fmb, ln_gain, ln_bias):
    emb_size = lax.axis_size("emb")
    dp_size = lax.axis_size("dp")
    rows, samples, width = embeddings.shape
    share = samples // emb_size
    emb_count = w_lcb.shape[1]
    group = 4 if share % 8 == 0 else 2 if share % 2 == 0 else 1
    x = embeddings.transpose(1, 0, 2)
    vmem = pl.BlockSpec(memory_space=pltpu.VMEM)
    y = pl.pallas_call(
        functools.partial(sample_kernel, emb_size, dp_size, group, 1e-05),
        out_shape=jax.ShapeDtypeStruct((samples, rows, width), jnp.bfloat16),
        in_specs=[vmem] * 4,
        out_specs=vmem,
        scratch_shapes=[
            pltpu.VMEM((share, emb_count, width), jnp.bfloat16),
            pltpu.VMEM((share, emb_count, width), jnp.bfloat16),
            pltpu.VMEM((emb_count, width), jnp.float32),
            pltpu.VMEM((emb_count, emb_count), jnp.bfloat16),
            pltpu.SemaphoreType.DMA((dp_size,)),
            pltpu.SemaphoreType.DMA((dp_size,)),
            pltpu.SemaphoreType.DMA((share // group, emb_size)),
            pltpu.SemaphoreType.DMA((share // group, emb_size)),
            pltpu.SemaphoreType.DMA((share // group, emb_size)),
            pltpu.SemaphoreType.DMA((share // group, emb_size)),
            pltpu.SemaphoreType.DMA(()),
        ],
        compiler_params=pltpu.CompilerParams(
            collective_id=0, has_side_effects=True, vmem_limit_bytes=40 * 1024 * 1024
        ),
    )(x, w_lcb, machine_projection.T, w_fmb)
    scaled = y.transpose(1, 0, 2).astype(jnp.float32)
    return (scaled * ln_gain[:, None, :] + ln_bias[:, None, :]).astype(jnp.bfloat16)


def tile_kernel(
    emb_size, dp_size, cores, eps,
    x_hbm, w_hbm, proj_hbm, fmb_hbm, gain_hbm, bias_hbm, y_ref,
    own, got, done, back, wide, spaced, mixed_ref, weights, factors, affine,
    w_send, w_recv, send_sem, in_recv, out_recv, load_sem, outer, beside, far,
):
    me = lax.axis_index("emb")
    mine = lax.axis_index("dp")
    chips = emb_size // cores
    chip = me // cores
    emb_count, share, width = got.shape
    rows = x_hbm.shape[0]
    w_rows = w_hbm.shape[0]
    block = rows * share
    others = emb_size - 1
    entries = float(emb_count * width)
    columns = [pl.ds(c, LANES) for c in range(0, width, LANES)]
    near = [sign * step for step in range(1, chips) for sign in (1, -1)]
    half = max(chips // 2, 1)
    dp_bits = [1 << i for i in range(dp_size.bit_length() - 1)]

    def inside(other):
        return (other >= 0) & (other < chips)

    def on_chip(step, action):
        other = chip + step

        @pl.when(inside(other))
        def _():
            for k in range(cores):
                peer = other * cores + k
                if step:
                    action(peer)
                else:
                    pl.when(peer != me)(functools.partial(action, peer))

    def same_side_then_across(action):
        for crossing in (False, True):
            for step in reversed(near) if crossing else near:
                other = chip + step
                across = (other // half) != (chip // half)

                @pl.when(inside(other) & (across if crossing else jnp.logical_not(across)))
                def _():
                    for k in range(cores):
                        action(other * cores + k)
            if not crossing:
                on_chip(0, action)

    def dp_partner(bit):
        return mine + bit * (1 - 2 * lax.rem(mine // bit, 2))

    def of_peer(ref, peer):
        return ref.at[:, pl.ds(pl.multiple_of(peer * share, share), share)]

    def signal(semaphore, peer):
        pl.semaphore_signal(semaphore, inc=1, device_id={"emb": peer}, device_id_type=MESH)

    inward = 1 - 2 * (chip // half if chips > 1 else chip)
    inward = jnp.maximum(inward, -1)
    middle = (chip == half - 1) | (chip == half)
    core = lax.rem(me, cores)
    neighbours = (me + inward * cores, me - inward * cores)
    there = (inside(chip + inward), inside(chip - inward))

    barrier = pltpu.get_barrier_semaphore()
    pl.when(there[0] & middle)(functools.partial(signal, barrier, neighbours[0]))
    pl.when(there[1])(functools.partial(signal, barrier, neighbours[1]))

    @pl.when(core == 0)
    def _():
        for bit in dp_bits:
            pl.semaphore_signal(barrier, inc=1, device_id={"dp": dp_partner(bit)}, device_id_type=MESH)

    @pl.when(core != 0)
    def _():
        signal(barrier, me - core)

    own_in = pltpu.make_async_copy(of_peer(x_hbm, me), own, load_sem.at[0])
    own_w = pltpu.make_async_copy(
        w_hbm, weights.at[pl.ds(pl.multiple_of(mine * w_rows, w_rows), w_rows)], load_sem.at[1]
    )

    def in_copy(source, peer):
        return pltpu.make_async_remote_copy(
            src_ref=of_peer(x_hbm, peer),
            dst_ref=got.at[pl.ds(source * rows, rows)],
            send_sem=send_sem,
            recv_sem=in_recv,
            device_id={"emb": peer},
            device_id_type=MESH,
        )

    def last_source(receiver):
        return jnp.where(receiver // cores < half, half, half - 1) * cores + cores - 1

    def out_copy(source, peer):
        return pltpu.make_async_remote_copy(
            src_ref=done.at[pl.ds(peer * rows, rows)],
            dst_ref=back.at[source],
            send_sem=send_sem,
            recv_sem=out_recv.at[(source == last_source(peer)).astype(jnp.int32)],
            device_id={"emb": peer},
            device_id_type=MESH,
        )

    def w_copy(i):
        bit = dp_bits[i]
        held = pl.multiple_of((mine // bit) * (bit * w_rows), bit * w_rows)
        part = weights.at[pl.ds(held, bit * w_rows)]
        return pltpu.make_async_remote_copy(
            src_ref=part,
            dst_ref=part,
            send_sem=w_send,
            recv_sem=w_recv.at[i],
            device_id={"dp": dp_partner(bit)},
            device_id_type=MESH,
        )

    def w_pass(peer):
        return pltpu.make_async_remote_copy(
            src_ref=weights,
            dst_ref=weights,
            send_sem=w_send,
            recv_sem=w_recv.at[0],
            device_id={"emb": peer},
            device_id_type=MESH,
        )

    def wait_for(ref, semaphore):
        pltpu.make_async_copy(ref, ref, semaphore).wait()

    def tell(distance):
        for sign in (1, -1):
            @pl.when(inside(chip + sign * (distance - 1)) & inside(chip - sign))
            def _():
                signal(far.at[distance - 2], me - sign * cores)

    def heard(distance):
        count = inside(chip + distance).astype(jnp.int32) + inside(chip - distance).astype(jnp.int32)

        @pl.when(count > 0)
        def _():
            pl.semaphore_wait(far.at[distance - 2], count)

    pl.semaphore_wait(
        barrier,
        there[0].astype(jnp.int32) + jnp.where(core == 0, cores - 1 + len(dp_bits), 0),
    )
    pl.when(there[0])(lambda: in_copy(me, neighbours[0]).start())
    own_in.start()
    pl.when(there[0] & jnp.logical_not(middle))(functools.partial(signal, outer, neighbours[0]))

    @pl.when(there[1])
    def _():
        pl.semaphore_wait(outer, 1)
        in_copy(me, neighbours[1]).start()

    @pl.when(core == 0)
    def _():
        own_w.start()
        for k in range(1, cores):
            signal(beside, me + k)
        if cores > 1:
            pl.semaphore_wait(beside, cores - 1)

    @pl.when(core != 0)
    def _():
        pl.semaphore_wait(beside, 1)
        signal(beside, me - core)

    for source, target in ((proj_hbm, factors.at[:, pl.ds(0, emb_count)]), (fmb_hbm, factors.at[:, pl.ds(emb_count, width)])):
        pltpu.make_async_copy(source, target, load_sem.at[2]).start()
    for i, source in enumerate((gain_hbm, bias_hbm)):
        pltpu.make_async_copy(source, affine.at[i], load_sem.at[3]).start()
    if chips > 2:
        tell(2)

    for k in range(cores):
        for distance in range(chips):
            if k == 0 and distance >= 2:
                heard(distance)
                if distance < chips - 1:
                    tell(distance + 1)
            for step in (distance, -distance) if distance else (0,):
                peer = (chip + step) * cores + k
                left = peer != me + step * cores if distance < 2 else True

                @pl.when(inside(chip + step) & left)
                def _():
                    in_copy(me, peer).start()

    @pl.when(core == 0)
    def _():
        own_w.wait()
        for i in range(len(dp_bits)):
            w_copy(i).start()
            w_copy(i).wait_recv()
        for k in range(1, cores):
            w_pass(me + k).start()

    @pl.when(core != 0)
    def _():
        w_pass(me - core).wait_recv()

    wait_for(factors, load_sem.at[2])
    wait_for(affine, load_sem.at[3])

    def widen(source, taken):
        taken = taken.astype(jnp.float32).reshape(block, width)
        for c in range(len(columns)):
            wide[c, pl.ds(pl.multiple_of(source * block, block), block)] = taken[:, c * LANES:(c + 1) * LANES]

    own_in.wait()
    widen(me, own[...])
    wait_for(got.at[pl.ds(0, others * rows)], in_recv)

    @pl.loop(0, emb_size)
    def _(source):
        @pl.when(source != me)
        def _():
            widen(source, got[pl.ds(source * rows, rows)])

    @pl.loop(0, share)
    def _(b):
        x = jnp.concatenate(
            [wide[c, pl.ds(b, emb_count, stride=share), :] for c in range(len(columns))], axis=1
        ).astype(jnp.bfloat16)
        factor = jnp.dot(
            factors[:, :emb_count], x, preferred_element_type=jnp.float32
        ).astype(jnp.bfloat16)
        inner = lax.dot_general(
            x, factor, (((1,), (1,)), ((), ())), preferred_element_type=jnp.float32
        ).astype(jnp.bfloat16)
        mixed_ref[...] = (
            jnp.dot(weights[...], x, preferred_element_type=jnp.float32)
            + jnp.dot(inner, factors[:, emb_count:], preferred_element_type=jnp.float32)
            + x.astype(jnp.float32)
        )
        mixed = mixed_ref[...]
        average = jnp.sum(mixed) / entries
        centered = mixed - average
        spread = jnp.sum(centered * centered) / entries
        scale = lax.rsqrt(jnp.full((1, width), spread + eps, jnp.float32))
        scaled = centered * scale
        for c in range(len(columns)):
            spaced[c, pl.ds(b, emb_count, stride=share), :] = scaled[:, c * LANES:(c + 1) * LANES]

    def narrow(target):
        for c, column in enumerate(columns):
            done[pl.ds(target * rows, rows), :, column] = (
                spaced[c, pl.ds(pl.multiple_of(target * block, block), block)]
                .reshape(rows, share, LANES)
                .astype(jnp.bfloat16)
            )

    def land(source, taken):
        y_ref[:, pl.ds(pl.multiple_of(source * share, share), share), :] = (
            taken.astype(jnp.float32) * affine[0][:, None, :] + affine[1][:, None, :]
        ).astype(jnp.bfloat16)

    pl.loop(0, emb_size)(narrow)
    land(me, done[pl.ds(me * rows, rows)])
    same_side_then_across(lambda peer: out_copy(me, peer).start())

    @pl.when(core == 0)
    def _():
        wait_for(weights.at[pl.ds(0, (dp_size - 1) * w_rows)], w_send)
        for k in range(1, cores):
            w_pass(me + k).wait_send()


    last = last_source(me)
    wait_for(back.at[pl.ds(0, others - 1)], out_recv.at[0])

    @pl.loop(0, emb_size)
    def _(source):
        @pl.when((source != me) & (source != last))
        def _():
            land(source, back[source])

    wait_for(back.at[0], out_recv.at[1])
    land(last, back[last])
    wait_for(wide.at[:, pl.ds(0, others * block)], send_sem)


def write_kernel(y_ref, out_ref, sem):
    copy = pltpu.make_async_copy(y_ref, out_ref, sem)
    copy.start()
    copy.wait()


def tile_body(embeddings, machine_projection, w_lcb, w_fmb, ln_gain, ln_bias):
    emb_size = lax.axis_size("emb")
    dp_size = lax.axis_size("dp")
    rows, samples, width = embeddings.shape
    share = samples // emb_size
    emb_count, rank = machine_projection.shape
    cores = 2 if emb_size % 2 == 0 else 1
    dma = pltpu.SemaphoreType.DMA
    y = pl.pallas_call(
        functools.partial(tile_kernel, emb_size, dp_size, cores, 1e-05),
        out_shape=pltpu.VMEM((rows, samples, width), jnp.bfloat16),
        in_specs=[pl.BlockSpec(memory_space=pltpu.HBM)] * 6,
        out_specs=pl.BlockSpec(memory_space=pltpu.VMEM),
        scratch_shapes=[
            pltpu.VMEM((rows, share, width), jnp.bfloat16),
            pltpu.VMEM((emb_count, share, width), jnp.bfloat16),
            pltpu.VMEM((emb_count, share, width), jnp.bfloat16),
            pltpu.VMEM((emb_size, rows, share, width), jnp.bfloat16),
            pltpu.VMEM((width // LANES, emb_count * share, LANES), jnp.float32),
            pltpu.VMEM((width // LANES, emb_count * share, LANES), jnp.float32),
            pltpu.VMEM((emb_count, width), jnp.float32),
            pltpu.VMEM((emb_count, emb_count), jnp.bfloat16),
            pltpu.VMEM((rank, emb_count + width), jnp.bfloat16),
            pltpu.VMEM((2, rows, width), jnp.float32),
            dma(()),
            dma((dp_size.bit_length() - 1,)),
            dma(()),
            dma(()),
            dma((2,)),
            dma((4,)),
            pltpu.SemaphoreType.REGULAR,
            pltpu.SemaphoreType.REGULAR,
            pltpu.SemaphoreType.REGULAR((max(emb_size // cores - 2, 1),)),
        ],
        compiler_params=pltpu.CompilerParams(
            collective_id=0, has_side_effects=True, vmem_limit_bytes=VMEM_LIMIT
        ),
    )(
        *(
            pltpu.with_memory_space_constraint(array, pltpu.HBM)
            for array in (embeddings, w_lcb, machine_projection.T, w_fmb, ln_gain, ln_bias)
        )
    )
    return pl.pallas_call(
        write_kernel,
        out_shape=jax.ShapeDtypeStruct(y.shape, y.dtype),
        in_specs=[pl.BlockSpec(memory_space=pltpu.VMEM)],
        out_specs=pl.BlockSpec(memory_space=pltpu.HBM),
        scratch_shapes=[dma(())],
        compiler_params=pltpu.CompilerParams(vmem_limit_bytes=4 * 1024 * 1024),
    )(y)


def body(embeddings, *rest):
    share = embeddings.shape[1] // lax.axis_size("emb")
    dp_size = lax.axis_size("dp")
    whole_tiles = share % 8 == 0 and lax.axis_size("emb") % 4 == 0 and dp_size > 1 and dp_size & (dp_size - 1) == 0
    return (tile_body if whole_tiles else sample_body)(embeddings, *rest)


def solution(mesh):
    return jax.shard_map(
        body,
        mesh=mesh,
        in_specs=(P("emb", "dp", None), P(), P("dp", None), P(), P("emb", None), P("emb", None)),
        out_specs=P("emb", "dp", None),
        check_vma=False,
    )
```

```python
import functools

import jax
import jax.numpy as jnp
from jax import lax
from jax.experimental import pallas as pl
from jax.experimental.pallas import tpu as pltpu
from jax.sharding import PartitionSpec as P

MESH = pl.DeviceIdType.MESH
LANES = 128
VMEM_LIMIT = 40 * 1024 * 1024


def sample_kernel(
    emb_size, dp_size, group, eps,
    x_ref, w_ref, proj_ref, fmb_ref, y_ref,
    got, done, mixed_ref, weights,
    w_send, w_recv, in_send, in_recv, out_send, out_recv, local_sem,
):
    me = lax.axis_index("emb")
    mine = lax.axis_index("dp")
    share = got.shape[0]
    rows = x_ref.shape[1]
    w_rows = w_ref.shape[0]
    entries = float(got.shape[1] * got.shape[2])
    emb_offsets = list(range(1, emb_size))
    dp_offsets = list(range(1, dp_size))

    barrier = pltpu.get_barrier_semaphore()
    for k in emb_offsets:
        pl.semaphore_signal(
            barrier, inc=1, device_id={"emb": lax.rem(me + k, emb_size)}, device_id_type=MESH
        )
    for k in dp_offsets:
        pl.semaphore_signal(
            barrier, inc=1, device_id={"dp": lax.rem(mine + k, dp_size)}, device_id_type=MESH
        )
    pl.semaphore_wait(barrier, len(emb_offsets) + len(dp_offsets))

    def w_copy(k):
        return pltpu.make_async_remote_copy(
            src_ref=w_ref,
            dst_ref=weights.at[pl.ds(pl.multiple_of(mine * w_rows, w_rows), w_rows)],
            send_sem=w_send.at[k],
            recv_sem=w_recv.at[k],
            device_id={"dp": lax.rem(mine + k, dp_size)},
            device_id_type=MESH,
        )

    def in_copy(c, k):
        peer = lax.rem(me + k, emb_size)
        return pltpu.make_async_remote_copy(
            src_ref=x_ref.at[pl.ds(peer * share + c * group, group)],
            dst_ref=got.at[pl.ds(c * group, group), pl.ds(pl.multiple_of(me * rows, rows), rows)],
            send_sem=in_send.at[c, k],
            recv_sem=in_recv.at[c, k],
            device_id={"emb": peer},
            device_id_type=MESH,
        )

    def out_copy(c, k):
        peer = lax.rem(me + k, emb_size)
        return pltpu.make_async_remote_copy(
            src_ref=done.at[pl.ds(c * group, group), pl.ds(pl.multiple_of(peer * rows, rows), rows)],
            dst_ref=y_ref.at[pl.ds(me * share + c * group, group)],
            send_sem=out_send.at[c, k],
            recv_sem=out_recv.at[c, k],
            device_id={"emb": peer},
            device_id_type=MESH,
        )

    def own_in(c):
        return pltpu.make_async_copy(
            x_ref.at[pl.ds(me * share + c * group, group)],
            got.at[pl.ds(c * group, group), pl.ds(pl.multiple_of(me * rows, rows), rows)],
            in_recv.at[c, 0],
        )

    def own_out(c):
        return pltpu.make_async_copy(
            done.at[pl.ds(c * group, group), pl.ds(pl.multiple_of(me * rows, rows), rows)],
            y_ref.at[pl.ds(me * share + c * group, group)],
            out_recv.at[c, 0],
        )

    own_w = pltpu.make_async_copy(
        w_ref, weights.at[pl.ds(pl.multiple_of(mine * w_rows, w_rows), w_rows)], local_sem
    )
    own_w.start()
    for k in dp_offsets:
        w_copy(k).start()

    @pl.loop(0, share // group)
    def _(c):
        for k in emb_offsets:
            in_copy(c, k).start()
        own_in(c).start()

    own_w.wait()
    for k in dp_offsets:
        w_copy(k).wait()

    @pl.loop(0, share // group)
    def _(c):
        own_in(c).wait()
        for k in emb_offsets:
            in_copy(c, k).wait_recv()

        @pl.loop(c * group, (c + 1) * group)
        def _(b):
            x = got[b]
            factor = jnp.dot(proj_ref[...], x, preferred_element_type=jnp.float32).astype(jnp.bfloat16)
            inner = lax.dot_general(
                x, factor, (((1,), (1,)), ((), ())), preferred_element_type=jnp.float32
            ).astype(jnp.bfloat16)
            mixed_ref[...] = (
                jnp.dot(weights[...], x, preferred_element_type=jnp.float32)
                + jnp.dot(inner, fmb_ref[...], preferred_element_type=jnp.float32)
                + x.astype(jnp.float32)
            )
            mixed = mixed_ref[...]
            average = jnp.sum(mixed) / entries
            centered = mixed - average
            spread = jnp.sum(centered * centered) / entries
            scale = lax.rsqrt(jnp.full((1, x.shape[1]), spread + eps, jnp.float32))
            done[b] = (centered * scale).astype(jnp.bfloat16)

        for k in emb_offsets:
            out_copy(c, k).start()
        own_out(c).start()

    @pl.loop(0, share // group)
    def _(c):
        own_out(c).wait()
        for k in emb_offsets:
            in_copy(c, k).wait_send()
            out_copy(c, k).wait()


def sample_body(embeddings, machine_projection, w_lcb, w_fmb, ln_gain, ln_bias):
    emb_size = lax.axis_size("emb")
    dp_size = lax.axis_size("dp")
    rows, samples, width = embeddings.shape
    share = samples // emb_size
    emb_count = w_lcb.shape[1]
    group = 4 if share % 8 == 0 else 2 if share % 2 == 0 else 1
    x = embeddings.transpose(1, 0, 2)
    vmem = pl.BlockSpec(memory_space=pltpu.VMEM)
    y = pl.pallas_call(
        functools.partial(sample_kernel, emb_size, dp_size, group, 1e-05),
        out_shape=jax.ShapeDtypeStruct((samples, rows, width), jnp.bfloat16),
        in_specs=[vmem] * 4,
        out_specs=vmem,
        scratch_shapes=[
            pltpu.VMEM((share, emb_count, width), jnp.bfloat16),
            pltpu.VMEM((share, emb_count, width), jnp.bfloat16),
            pltpu.VMEM((emb_count, width), jnp.float32),
            pltpu.VMEM((emb_count, emb_count), jnp.bfloat16),
            pltpu.SemaphoreType.DMA((dp_size,)),
            pltpu.SemaphoreType.DMA((dp_size,)),
            pltpu.SemaphoreType.DMA((share // group, emb_size)),
            pltpu.SemaphoreType.DMA((share // group, emb_size)),
            pltpu.SemaphoreType.DMA((share // group, emb_size)),
            pltpu.SemaphoreType.DMA((share // group, emb_size)),
            pltpu.SemaphoreType.DMA(()),
        ],
        compiler_params=pltpu.CompilerParams(
            collective_id=0, has_side_effects=True, vmem_limit_bytes=40 * 1024 * 1024
        ),
    )(x, w_lcb, machine_projection.T, w_fmb)
    scaled = y.transpose(1, 0, 2).astype(jnp.float32)
    return (scaled * ln_gain[:, None, :] + ln_bias[:, None, :]).astype(jnp.bfloat16)


def tile_kernel(
    emb_size, dp_size, cores, eps,
    x_hbm, w_hbm, proj_hbm, fmb_hbm, gain_hbm, bias_hbm, y_ref,
    own, got, done, back, wide, spaced, mixed_ref, weights, factors, affine,
    w_send, w_recv, send_sem, in_recv, out_recv, load_sem, outer, beside, far,
):
    me = lax.axis_index("emb")
    mine = lax.axis_index("dp")
    chips = emb_size // cores
    chip = me // cores
    emb_count, share, width = got.shape
    rows = x_hbm.shape[0]
    w_rows = w_hbm.shape[0]
    block = rows * share
    others = emb_size - 1
    entries = float(emb_count * width)
    columns = [pl.ds(c, LANES) for c in range(0, width, LANES)]
    near = [sign * step for step in range(1, chips) for sign in (1, -1)]
    half = max(chips // 2, 1)
    dp_bits = [1 << i for i in range(dp_size.bit_length() - 1)]

    def inside(other):
        return (other >= 0) & (other < chips)

    def on_chip(step, action):
        other = chip + step

        @pl.when(inside(other))
        def _():
            for k in range(cores):
                peer = other * cores + k
                if step:
                    action(peer)
                else:
                    pl.when(peer != me)(functools.partial(action, peer))

    def same_side_then_across(action):
        for crossing in (False, True):
            for step in reversed(near) if crossing else near:
                other = chip + step
                across = (other // half) != (chip // half)

                @pl.when(inside(other) & (across if crossing else jnp.logical_not(across)))
                def _():
                    for k in range(cores):
                        action(other * cores + k)
            if not crossing:
                on_chip(0, action)

    def dp_partner(bit):
        return mine + bit * (1 - 2 * lax.rem(mine // bit, 2))

    def of_peer(ref, peer):
        return ref.at[:, pl.ds(pl.multiple_of(peer * share, share), share)]

    def signal(semaphore, peer):
        pl.semaphore_signal(semaphore, inc=1, device_id={"emb": peer}, device_id_type=MESH)

    inward = 1 - 2 * (chip // half if chips > 1 else chip)
    inward = jnp.maximum(inward, -1)
    middle = (chip == half - 1) | (chip == half)
    core = lax.rem(me, cores)
    neighbours = (me + inward * cores, me - inward * cores)
    there = (inside(chip + inward), inside(chip - inward))

    barrier = pltpu.get_barrier_semaphore()
    pl.when(there[0] & middle)(functools.partial(signal, barrier, neighbours[0]))
    pl.when(there[1])(functools.partial(signal, barrier, neighbours[1]))

    @pl.when(core == 0)
    def _():
        for bit in dp_bits:
            pl.semaphore_signal(barrier, inc=1, device_id={"dp": dp_partner(bit)}, device_id_type=MESH)

    @pl.when(core != 0)
    def _():
        signal(barrier, me - core)

    own_in = pltpu.make_async_copy(of_peer(x_hbm, me), own, load_sem.at[0])
    own_w = pltpu.make_async_copy(
        w_hbm, weights.at[pl.ds(pl.multiple_of(mine * w_rows, w_rows), w_rows)], load_sem.at[1]
    )

    def in_copy(source, peer):
        return pltpu.make_async_remote_copy(
            src_ref=of_peer(x_hbm, peer),
            dst_ref=got.at[pl.ds(source * rows, rows)],
            send_sem=send_sem,
            recv_sem=in_recv,
            device_id={"emb": peer},
            device_id_type=MESH,
        )

    def last_source(receiver):
        return jnp.where(receiver // cores < half, half, half - 1) * cores + cores - 1

    def out_copy(source, peer):
        return pltpu.make_async_remote_copy(
            src_ref=done.at[pl.ds(peer * rows, rows)],
            dst_ref=back.at[source],
            send_sem=send_sem,
            recv_sem=out_recv.at[(source == last_source(peer)).astype(jnp.int32)],
            device_id={"emb": peer},
            device_id_type=MESH,
        )

    def w_copy(i):
        bit = dp_bits[i]
        held = pl.multiple_of((mine // bit) * (bit * w_rows), bit * w_rows)
        part = weights.at[pl.ds(held, bit * w_rows)]
        return pltpu.make_async_remote_copy(
            src_ref=part,
            dst_ref=part,
            send_sem=w_send,
            recv_sem=w_recv.at[i],
            device_id={"dp": dp_partner(bit)},
            device_id_type=MESH,
        )

    def w_pass(peer):
        return pltpu.make_async_remote_copy(
            src_ref=weights,
            dst_ref=weights,
            send_sem=w_send,
            recv_sem=w_recv.at[0],
            device_id={"emb": peer},
            device_id_type=MESH,
        )

    def wait_for(ref, semaphore):
        pltpu.make_async_copy(ref, ref, semaphore).wait()

    def tell(distance):
        for sign in (1, -1):
            @pl.when(inside(chip + sign * (distance - 1)) & inside(chip - sign))
            def _():
                signal(far.at[distance - 2], me - sign * cores)

    def heard(distance):
        count = inside(chip + distance).astype(jnp.int32) + inside(chip - distance).astype(jnp.int32)

        @pl.when(count > 0)
        def _():
            pl.semaphore_wait(far.at[distance - 2], count)

    pl.semaphore_wait(
        barrier,
        there[0].astype(jnp.int32) + jnp.where(core == 0, cores - 1 + len(dp_bits), 0),
    )
    pl.when(there[0])(lambda: in_copy(me, neighbours[0]).start())
    own_in.start()
    pl.when(there[0] & jnp.logical_not(middle))(functools.partial(signal, outer, neighbours[0]))

    @pl.when(there[1])
    def _():
        pl.semaphore_wait(outer, 1)
        in_copy(me, neighbours[1]).start()

    @pl.when(core == 0)
    def _():
        own_w.start()
        for k in range(1, cores):
            signal(beside, me + k)
        if cores > 1:
            pl.semaphore_wait(beside, cores - 1)

    @pl.when(core != 0)
    def _():
        pl.semaphore_wait(beside, 1)
        signal(beside, me - core)

    for source, first in ((proj_hbm, 0), (fmb_hbm, emb_count)):
        target = factors.at[:, pl.ds(first, source.shape[1])]
        pltpu.make_async_copy(source, target, load_sem.at[2]).start()
    for i, source in enumerate((gain_hbm, bias_hbm)):
        pltpu.make_async_copy(source, affine.at[i], load_sem.at[3]).start()
    if chips > 2:
        tell(2)

    for k in range(cores):
        for distance in range(chips):
            if k == 0 and distance >= 2:
                heard(distance)
                if distance < chips - 1:
                    tell(distance + 1)
            for step in (distance, -distance) if distance else (0,):
                peer = (chip + step) * cores + k
                left = peer != me + step * cores if distance < 2 else True

                @pl.when(inside(chip + step) & left)
                def _():
                    in_copy(me, peer).start()

    @pl.when(core == 0)
    def _():
        own_w.wait()
        for i in range(len(dp_bits)):
            w_copy(i).start()
            w_copy(i).wait_recv()
        for k in range(1, cores):
            w_pass(me + k).start()

    @pl.when(core != 0)
    def _():
        w_pass(me - core).wait_recv()

    wait_for(factors, load_sem.at[2])
    wait_for(affine, load_sem.at[3])

    def widen(source, taken):
        taken = taken.astype(jnp.float32).reshape(block, width)
        for c in range(len(columns)):
            wide[c, pl.ds(pl.multiple_of(source * block, block), block)] = taken[:, c * LANES:(c + 1) * LANES]

    own_in.wait()
    widen(me, own[...])
    wait_for(got.at[pl.ds(0, others * rows)], in_recv)

    @pl.loop(0, emb_size)
    def _(source):
        @pl.when(source != me)
        def _():
            widen(source, got[pl.ds(source * rows, rows)])

    @pl.loop(0, share)
    def _(b):
        x = jnp.concatenate(
            [wide[c, pl.ds(b, emb_count, stride=share), :] for c in range(len(columns))], axis=1
        ).astype(jnp.bfloat16)
        factor = jnp.dot(
            factors[:, :emb_count], x, preferred_element_type=jnp.float32
        ).astype(jnp.bfloat16)
        inner = lax.dot_general(
            x, factor, (((1,), (1,)), ((), ())), preferred_element_type=jnp.float32
        ).astype(jnp.bfloat16)
        mixed_ref[...] = (
            jnp.dot(weights[...], x, preferred_element_type=jnp.float32)
            + jnp.dot(inner, factors[:, emb_count:], preferred_element_type=jnp.float32)
            + x.astype(jnp.float32)
        )
        mixed = mixed_ref[...]
        average = jnp.sum(mixed) / entries
        centered = mixed - average
        spread = jnp.sum(centered * centered) / entries
        scale = lax.rsqrt(jnp.full((1, width), spread + eps, jnp.float32))
        scaled = centered * scale
        for c in range(len(columns)):
            spaced[c, pl.ds(b, emb_count, stride=share), :] = scaled[:, c * LANES:(c + 1) * LANES]

    def narrow(target):
        for c, column in enumerate(columns):
            done[pl.ds(target * rows, rows), :, column] = (
                spaced[c, pl.ds(pl.multiple_of(target * block, block), block)]
                .reshape(rows, share, LANES)
                .astype(jnp.bfloat16)
            )

    def land(source, taken):
        y_ref[:, pl.ds(pl.multiple_of(source * share, share), share), :] = (
            taken.astype(jnp.float32) * affine[0][:, None, :] + affine[1][:, None, :]
        ).astype(jnp.bfloat16)

    pl.loop(0, emb_size)(narrow)
    land(me, done[pl.ds(me * rows, rows)])
    same_side_then_across(lambda peer: out_copy(me, peer).start())

    @pl.when(core == 0)
    def _():
        wait_for(weights.at[pl.ds(0, (dp_size - 1) * w_rows)], w_send)
        for k in range(1, cores):
            w_pass(me + k).wait_send()

    last = last_source(me)
    wait_for(back.at[pl.ds(0, others - 1)], out_recv.at[0])

    @pl.loop(0, emb_size)
    def _(source):
        @pl.when((source != me) & (source != last))
        def _():
            land(source, back[source])

    wait_for(back.at[0], out_recv.at[1])
    land(last, back[last])
    wait_for(wide.at[:, pl.ds(0, others * block)], send_sem)


def tile_body(embeddings, machine_projection, w_lcb, w_fmb, ln_gain, ln_bias):
    emb_size = lax.axis_size("emb")
    dp_size = lax.axis_size("dp")
    rows, samples, width = embeddings.shape
    share = samples // emb_size
    emb_count, rank = machine_projection.shape
    cores = 2 if emb_size % 2 == 0 else 1
    dma = pltpu.SemaphoreType.DMA
    return pl.pallas_call(
        functools.partial(tile_kernel, emb_size, dp_size, cores, 1e-05),
        out_shape=pltpu.VMEM((rows, samples, width), jnp.bfloat16),
        in_specs=[pl.BlockSpec(memory_space=pltpu.HBM)] * 6,
        out_specs=pl.BlockSpec(memory_space=pltpu.VMEM),
        scratch_shapes=[
            pltpu.VMEM((rows, share, width), jnp.bfloat16),
            pltpu.VMEM((emb_count, share, width), jnp.bfloat16),
            pltpu.VMEM((emb_count, share, width), jnp.bfloat16),
            pltpu.VMEM((emb_size, rows, share, width), jnp.bfloat16),
            pltpu.VMEM((width // LANES, emb_count * share, LANES), jnp.float32),
            pltpu.VMEM((width // LANES, emb_count * share, LANES), jnp.float32),
            pltpu.VMEM((emb_count, width), jnp.float32),
            pltpu.VMEM((emb_count, emb_count), jnp.bfloat16),
            pltpu.VMEM((rank, emb_count + width), jnp.bfloat16),
            pltpu.VMEM((2, rows, width), jnp.float32),
            dma(()),
            dma((dp_size.bit_length() - 1,)),
            dma(()),
            dma(()),
            dma((2,)),
            dma((4,)),
            pltpu.SemaphoreType.REGULAR,
            pltpu.SemaphoreType.REGULAR,
            pltpu.SemaphoreType.REGULAR((max(emb_size // cores - 2, 1),)),
        ],
        compiler_params=pltpu.CompilerParams(
            collective_id=0, has_side_effects=True, vmem_limit_bytes=VMEM_LIMIT
        ),
    )(
        *(
            pltpu.with_memory_space_constraint(array, pltpu.HBM)
            for array in (embeddings, w_lcb, machine_projection.T, w_fmb, ln_gain, ln_bias)
        )
    )


def body(embeddings, *rest):
    share = embeddings.shape[1] // lax.axis_size("emb")
    dp_size = lax.axis_size("dp")
    whole_tiles = share % 8 == 0 and lax.axis_size("emb") % 4 == 0 and dp_size > 1 and dp_size & (dp_size - 1) == 0
    return (tile_body if whole_tiles else sample_body)(embeddings, *rest)


def solution(mesh):
    return jax.shard_map(
        body,
        mesh=mesh,
        in_specs=(P("emb", "dp", None), P(), P("dp", None), P(), P("emb", None), P("emb", None)),
        out_specs=P("emb", "dp", None),
        check_vma=False,
    )
```

```python
import functools

import jax
import jax.numpy as jnp
from jax import lax
from jax.experimental import pallas as pl
from jax.experimental.pallas import tpu as pltpu
from jax.sharding import PartitionSpec as P

MESH = pl.DeviceIdType.MESH
LANES = 128
VMEM_LIMIT = 40 * 1024 * 1024


def sample_kernel(
    emb_size, dp_size, group, eps,
    x_ref, w_ref, proj_ref, fmb_ref, y_ref,
    got, done, mixed_ref, weights,
    w_send, w_recv, in_send, in_recv, out_send, out_recv, local_sem,
):
    me = lax.axis_index("emb")
    mine = lax.axis_index("dp")
    share = got.shape[0]
    rows = x_ref.shape[1]
    w_rows = w_ref.shape[0]
    entries = float(got.shape[1] * got.shape[2])
    emb_offsets = list(range(1, emb_size))
    dp_offsets = list(range(1, dp_size))

    barrier = pltpu.get_barrier_semaphore()
    for k in emb_offsets:
        pl.semaphore_signal(
            barrier, inc=1, device_id={"emb": lax.rem(me + k, emb_size)}, device_id_type=MESH
        )
    for k in dp_offsets:
        pl.semaphore_signal(
            barrier, inc=1, device_id={"dp": lax.rem(mine + k, dp_size)}, device_id_type=MESH
        )
    pl.semaphore_wait(barrier, len(emb_offsets) + len(dp_offsets))

    def w_copy(k):
        return pltpu.make_async_remote_copy(
            src_ref=w_ref,
            dst_ref=weights.at[pl.ds(pl.multiple_of(mine * w_rows, w_rows), w_rows)],
            send_sem=w_send.at[k],
            recv_sem=w_recv.at[k],
            device_id={"dp": lax.rem(mine + k, dp_size)},
            device_id_type=MESH,
        )

    def in_copy(c, k):
        peer = lax.rem(me + k, emb_size)
        return pltpu.make_async_remote_copy(
            src_ref=x_ref.at[pl.ds(peer * share + c * group, group)],
            dst_ref=got.at[pl.ds(c * group, group), pl.ds(pl.multiple_of(me * rows, rows), rows)],
            send_sem=in_send.at[c, k],
            recv_sem=in_recv.at[c, k],
            device_id={"emb": peer},
            device_id_type=MESH,
        )

    def out_copy(c, k):
        peer = lax.rem(me + k, emb_size)
        return pltpu.make_async_remote_copy(
            src_ref=done.at[pl.ds(c * group, group), pl.ds(pl.multiple_of(peer * rows, rows), rows)],
            dst_ref=y_ref.at[pl.ds(me * share + c * group, group)],
            send_sem=out_send.at[c, k],
            recv_sem=out_recv.at[c, k],
            device_id={"emb": peer},
            device_id_type=MESH,
        )

    def own_in(c):
        return pltpu.make_async_copy(
            x_ref.at[pl.ds(me * share + c * group, group)],
            got.at[pl.ds(c * group, group), pl.ds(pl.multiple_of(me * rows, rows), rows)],
            in_recv.at[c, 0],
        )

    def own_out(c):
        return pltpu.make_async_copy(
            done.at[pl.ds(c * group, group), pl.ds(pl.multiple_of(me * rows, rows), rows)],
            y_ref.at[pl.ds(me * share + c * group, group)],
            out_recv.at[c, 0],
        )

    own_w = pltpu.make_async_copy(
        w_ref, weights.at[pl.ds(pl.multiple_of(mine * w_rows, w_rows), w_rows)], local_sem
    )
    own_w.start()
    for k in dp_offsets:
        w_copy(k).start()

    @pl.loop(0, share // group)
    def _(c):
        for k in emb_offsets:
            in_copy(c, k).start()
        own_in(c).start()

    own_w.wait()
    for k in dp_offsets:
        w_copy(k).wait()

    @pl.loop(0, share // group)
    def _(c):
        own_in(c).wait()
        for k in emb_offsets:
            in_copy(c, k).wait_recv()

        @pl.loop(c * group, (c + 1) * group)
        def _(b):
            x = got[b]
            factor = jnp.dot(proj_ref[...], x, preferred_element_type=jnp.float32).astype(jnp.bfloat16)
            inner = lax.dot_general(
                x, factor, (((1,), (1,)), ((), ())), preferred_element_type=jnp.float32
            ).astype(jnp.bfloat16)
            mixed_ref[...] = (
                jnp.dot(weights[...], x, preferred_element_type=jnp.float32)
                + jnp.dot(inner, fmb_ref[...], preferred_element_type=jnp.float32)
                + x.astype(jnp.float32)
            )
            mixed = mixed_ref[...]
            average = jnp.sum(mixed) / entries
            centered = mixed - average
            spread = jnp.sum(centered * centered) / entries
            scale = lax.rsqrt(jnp.full((1, x.shape[1]), spread + eps, jnp.float32))
            done[b] = (centered * scale).astype(jnp.bfloat16)

        for k in emb_offsets:
            out_copy(c, k).start()
        own_out(c).start()

    @pl.loop(0, share // group)
    def _(c):
        own_out(c).wait()
        for k in emb_offsets:
            in_copy(c, k).wait_send()
            out_copy(c, k).wait()


def sample_body(embeddings, machine_projection, w_lcb, w_fmb, ln_gain, ln_bias):
    emb_size = lax.axis_size("emb")
    dp_size = lax.axis_size("dp")
    rows, samples, width = embeddings.shape
    share = samples // emb_size
    emb_count = w_lcb.shape[1]
    group = 4 if share % 8 == 0 else 2 if share % 2 == 0 else 1
    x = embeddings.transpose(1, 0, 2)
    vmem = pl.BlockSpec(memory_space=pltpu.VMEM)
    y = pl.pallas_call(
        functools.partial(sample_kernel, emb_size, dp_size, group, 1e-05),
        out_shape=jax.ShapeDtypeStruct((samples, rows, width), jnp.bfloat16),
        in_specs=[vmem] * 4,
        out_specs=vmem,
        scratch_shapes=[
            pltpu.VMEM((share, emb_count, width), jnp.bfloat16),
            pltpu.VMEM((share, emb_count, width), jnp.bfloat16),
            pltpu.VMEM((emb_count, width), jnp.float32),
            pltpu.VMEM((emb_count, emb_count), jnp.bfloat16),
            pltpu.SemaphoreType.DMA((dp_size,)),
            pltpu.SemaphoreType.DMA((dp_size,)),
            pltpu.SemaphoreType.DMA((share // group, emb_size)),
            pltpu.SemaphoreType.DMA((share // group, emb_size)),
            pltpu.SemaphoreType.DMA((share // group, emb_size)),
            pltpu.SemaphoreType.DMA((share // group, emb_size)),
            pltpu.SemaphoreType.DMA(()),
        ],
        compiler_params=pltpu.CompilerParams(
            collective_id=0, has_side_effects=True, vmem_limit_bytes=40 * 1024 * 1024
        ),
    )(x, w_lcb, machine_projection.T, w_fmb)
    scaled = y.transpose(1, 0, 2).astype(jnp.float32)
    return (scaled * ln_gain[:, None, :] + ln_bias[:, None, :]).astype(jnp.bfloat16)


def tile_kernel(
    emb_size, dp_size, cores, eps,
    x_hbm, w_hbm, proj_hbm, fmb_hbm, gain_hbm, bias_hbm, y_ref,
    own, got, done, back, wide, spaced, mixed_ref, weights, factors, affine,
    w_send, w_recv, send_sem, in_recv, out_recv, load_sem, outer, beside, far,
):
    me = lax.axis_index("emb")
    mine = lax.axis_index("dp")
    chips = emb_size // cores
    chip = me // cores
    emb_count, share, width = got.shape
    rows = x_hbm.shape[0]
    w_rows = w_hbm.shape[0]
    block = rows * share
    others = emb_size - 1
    entries = float(emb_count * width)
    columns = [pl.ds(c, LANES) for c in range(0, width, LANES)]
    near = [sign * step for step in range(1, chips) for sign in (1, -1)]
    half = max(chips // 2, 1)
    dp_bits = [1 << i for i in range(dp_size.bit_length() - 1)]

    def inside(other):
        return (other >= 0) & (other < chips)

    def on_chip(step, action):
        other = chip + step

        @pl.when(inside(other))
        def _():
            for k in range(cores):
                peer = other * cores + k
                if step:
                    action(peer)
                else:
                    pl.when(peer != me)(functools.partial(action, peer))

    def same_side_then_across(action):
        for crossing in (False, True):
            for step in reversed(near) if crossing else near:
                other = chip + step
                across = (other // half) != (chip // half)

                @pl.when(inside(other) & (across if crossing else jnp.logical_not(across)))
                def _():
                    for k in range(cores):
                        action(other * cores + k)
            if not crossing:
                on_chip(0, action)

    def dp_partner(bit):
        return mine + bit * (1 - 2 * lax.rem(mine // bit, 2))

    def of_peer(ref, peer):
        return ref.at[:, pl.ds(pl.multiple_of(peer * share, share), share)]

    def signal(semaphore, peer):
        pl.semaphore_signal(semaphore, inc=1, device_id={"emb": peer}, device_id_type=MESH)

    inward = 1 - 2 * (chip // half if chips > 1 else chip)
    inward = jnp.maximum(inward, -1)
    middle = (chip == half - 1) | (chip == half)
    core = lax.rem(me, cores)
    neighbours = (me + inward * cores, me - inward * cores)
    there = (inside(chip + inward), inside(chip - inward))

    barrier = pltpu.get_barrier_semaphore()
    pl.when(there[0] & middle)(functools.partial(signal, barrier, neighbours[0]))
    pl.when(there[1])(functools.partial(signal, barrier, neighbours[1]))

    @pl.when(core == 0)
    def _():
        for bit in dp_bits:
            pl.semaphore_signal(barrier, inc=1, device_id={"dp": dp_partner(bit)}, device_id_type=MESH)

    @pl.when(core != 0)
    def _():
        signal(barrier, me - core)

    own_in = pltpu.make_async_copy(of_peer(x_hbm, me), own, load_sem.at[0])
    own_w = pltpu.make_async_copy(
        w_hbm, weights.at[pl.ds(pl.multiple_of(mine * w_rows, w_rows), w_rows)], load_sem.at[1]
    )

    def in_copy(source, peer):
        return pltpu.make_async_remote_copy(
            src_ref=of_peer(x_hbm, peer),
            dst_ref=got.at[pl.ds(source * rows, rows)],
            send_sem=send_sem,
            recv_sem=in_recv,
            device_id={"emb": peer},
            device_id_type=MESH,
        )

    def last_source(receiver):
        return jnp.where(receiver // cores < half, half, half - 1) * cores + cores - 1

    tail = max(rows // 8, 1)
    parts = ((0, rows - tail), (rows - tail, tail))

    def out_copy(source, peer, start=0, size=rows, slot=0):
        return pltpu.make_async_remote_copy(
            src_ref=done.at[pl.ds(peer * rows + start, size)],
            dst_ref=back.at[source, pl.ds(start, size)],
            send_sem=send_sem,
            recv_sem=out_recv.at[slot],
            device_id={"emb": peer},
            device_id_type=MESH,
        )

    def send_back(peer):
        ends = me == last_source(peer)
        pl.when(jnp.logical_not(ends))(lambda: out_copy(me, peer).start())

        @pl.when(ends)
        def _():
            for slot, (start, size) in enumerate(parts, 1):
                out_copy(me, peer, start, size, slot).start()

    def w_copy(i):
        bit = dp_bits[i]
        held = pl.multiple_of((mine // bit) * (bit * w_rows), bit * w_rows)
        part = weights.at[pl.ds(held, bit * w_rows)]
        return pltpu.make_async_remote_copy(
            src_ref=part,
            dst_ref=part,
            send_sem=w_send,
            recv_sem=w_recv.at[i],
            device_id={"dp": dp_partner(bit)},
            device_id_type=MESH,
        )

    def w_pass(peer):
        return pltpu.make_async_remote_copy(
            src_ref=weights,
            dst_ref=weights,
            send_sem=w_send,
            recv_sem=w_recv.at[0],
            device_id={"emb": peer},
            device_id_type=MESH,
        )

    def wait_for(ref, semaphore):
        pltpu.make_async_copy(ref, ref, semaphore).wait()

    def tell(distance):
        for sign in (1, -1):
            @pl.when(inside(chip + sign * (distance - 1)) & inside(chip - sign))
            def _():
                signal(far.at[distance - 2], me - sign * cores)

    def heard(distance):
        count = inside(chip + distance).astype(jnp.int32) + inside(chip - distance).astype(jnp.int32)

        @pl.when(count > 0)
        def _():
            pl.semaphore_wait(far.at[distance - 2], count)

    pl.semaphore_wait(
        barrier,
        there[0].astype(jnp.int32) + jnp.where(core == 0, cores - 1 + len(dp_bits), 0),
    )
    pl.when(there[0])(lambda: in_copy(me, neighbours[0]).start())
    own_in.start()
    pl.when(there[0] & jnp.logical_not(middle))(functools.partial(signal, outer, neighbours[0]))

    @pl.when(there[1])
    def _():
        pl.semaphore_wait(outer, 1)
        in_copy(me, neighbours[1]).start()

    @pl.when(core == 0)
    def _():
        own_w.start()
        for k in range(1, cores):
            signal(beside, me + k)
        if cores > 1:
            pl.semaphore_wait(beside, cores - 1)

    @pl.when(core != 0)
    def _():
        pl.semaphore_wait(beside, 1)
        signal(beside, me - core)

    for source, first in ((proj_hbm, 0), (fmb_hbm, emb_count)):
        target = factors.at[:, pl.ds(first, source.shape[1])]
        pltpu.make_async_copy(source, target, load_sem.at[0]).start()
    for i, source in enumerate((gain_hbm, bias_hbm)):
        pltpu.make_async_copy(source, affine.at[i], load_sem.at[0]).start()
    if chips > 2:
        tell(2)

    for k in range(cores):
        for distance in range(chips):
            if k == 0 and distance >= 2:
                heard(distance)
                if distance < chips - 1:
                    tell(distance + 1)
            for step in (distance, -distance) if distance else (0,):
                peer = (chip + step) * cores + k
                left = peer != me + step * cores if distance < 2 else True

                @pl.when(inside(chip + step) & left)
                def _():
                    in_copy(me, peer).start()

    @pl.when(core == 0)
    def _():
        own_w.wait()
        for i in range(len(dp_bits)):
            w_copy(i).start()
            w_copy(i).wait_recv()
        for k in range(1, cores):
            w_pass(me + k).start()

    @pl.when(core != 0)
    def _():
        w_pass(me - core).wait_recv()

    loaded = 2 * (own.size + factors.size) + 4 * affine.size
    wait_for(wide.at[0, pl.ds(0, loaded // (4 * LANES))], load_sem.at[0])

    def widen(source, taken):
        taken = taken.astype(jnp.float32).reshape(block, width)
        for c in range(len(columns)):
            wide[c, pl.ds(pl.multiple_of(source * block, block), block)] = taken[:, c * LANES:(c + 1) * LANES]

    widen(me, own[...])
    wait_for(got.at[pl.ds(0, others * rows)], in_recv)

    @pl.loop(0, emb_size)
    def _(source):
        @pl.when(source != me)
        def _():
            widen(source, got[pl.ds(source * rows, rows)])

    @pl.loop(0, share)
    def _(b):
        x = jnp.concatenate(
            [wide[c, pl.ds(b, emb_count, stride=share), :] for c in range(len(columns))], axis=1
        ).astype(jnp.bfloat16)
        factor = jnp.dot(
            factors[:, :emb_count], x, preferred_element_type=jnp.float32
        ).astype(jnp.bfloat16)
        inner = lax.dot_general(
            x, factor, (((1,), (1,)), ((), ())), preferred_element_type=jnp.float32
        ).astype(jnp.bfloat16)
        mixed_ref[...] = (
            jnp.dot(weights[...], x, preferred_element_type=jnp.float32)
            + jnp.dot(inner, factors[:, emb_count:], preferred_element_type=jnp.float32)
            + x.astype(jnp.float32)
        )
        mixed = mixed_ref[...]
        average = jnp.sum(mixed) / entries
        centered = mixed - average
        spread = jnp.sum(centered * centered) / entries
        scale = lax.rsqrt(jnp.full((1, width), spread + eps, jnp.float32))
        scaled = centered * scale
        for c in range(len(columns)):
            spaced[c, pl.ds(b, emb_count, stride=share), :] = scaled[:, c * LANES:(c + 1) * LANES]

    def narrow(target):
        for c, column in enumerate(columns):
            done[pl.ds(target * rows, rows), :, column] = (
                spaced[c, pl.ds(pl.multiple_of(target * block, block), block)]
                .reshape(rows, share, LANES)
                .astype(jnp.bfloat16)
            )

    def land(source, taken, start=0):
        part = pl.ds(start, taken.shape[0])
        y_ref[part, pl.ds(pl.multiple_of(source * share, share), share), :] = (
            taken.astype(jnp.float32) * affine[0, part][:, None, :] + affine[1, part][:, None, :]
        ).astype(jnp.bfloat16)

    pl.loop(0, emb_size)(narrow)
    land(me, done[pl.ds(me * rows, rows)])
    same_side_then_across(send_back)

    @pl.when(core == 0)
    def _():
        wait_for(weights.at[pl.ds(0, (dp_size - 1) * w_rows)], w_send)
        for k in range(1, cores):
            w_pass(me + k).wait_send()

    last = last_source(me)
    wait_for(back.at[pl.ds(0, others - 1)], out_recv.at[0])

    @pl.loop(0, emb_size)
    def _(source):
        @pl.when((source != me) & (source != last))
        def _():
            land(source, back[source])

    for slot, (start, size) in enumerate(parts, 1):
        wait_for(back.at[0, pl.ds(start, size)], out_recv.at[slot])
        land(last, back[last, pl.ds(start, size)], start)
    wait_for(wide.at[:, pl.ds(0, others * block)], send_sem)


def tile_body(embeddings, machine_projection, w_lcb, w_fmb, ln_gain, ln_bias):
    emb_size = lax.axis_size("emb")
    dp_size = lax.axis_size("dp")
    rows, samples, width = embeddings.shape
    share = samples // emb_size
    emb_count, rank = machine_projection.shape
    cores = 2 if emb_size % 2 == 0 else 1
    dma = pltpu.SemaphoreType.DMA
    return pl.pallas_call(
        functools.partial(tile_kernel, emb_size, dp_size, cores, 1e-05),
        out_shape=pltpu.VMEM((rows, samples, width), jnp.bfloat16),
        in_specs=[pl.BlockSpec(memory_space=pltpu.HBM)] * 6,
        out_specs=pl.BlockSpec(memory_space=pltpu.VMEM),
        scratch_shapes=[
            pltpu.VMEM((rows, share, width), jnp.bfloat16),
            pltpu.VMEM((emb_count, share, width), jnp.bfloat16),
            pltpu.VMEM((emb_count, share, width), jnp.bfloat16),
            pltpu.VMEM((emb_size, rows, share, width), jnp.bfloat16),
            pltpu.VMEM((width // LANES, emb_count * share, LANES), jnp.float32),
            pltpu.VMEM((width // LANES, emb_count * share, LANES), jnp.float32),
            pltpu.VMEM((emb_count, width), jnp.float32),
            pltpu.VMEM((emb_count, emb_count), jnp.bfloat16),
            pltpu.VMEM((rank, emb_count + width), jnp.bfloat16),
            pltpu.VMEM((2, rows, width), jnp.float32),
            dma(()),
            dma((dp_size.bit_length() - 1,)),
            dma(()),
            dma(()),
            dma((3,)),
            dma((2,)),
            pltpu.SemaphoreType.REGULAR,
            pltpu.SemaphoreType.REGULAR,
            pltpu.SemaphoreType.REGULAR((max(emb_size // cores - 2, 1),)),
        ],
        compiler_params=pltpu.CompilerParams(
            collective_id=0, has_side_effects=True, vmem_limit_bytes=VMEM_LIMIT
        ),
    )(
        *(
            pltpu.with_memory_space_constraint(array, pltpu.HBM)
            for array in (embeddings, w_lcb, machine_projection.T, w_fmb, ln_gain, ln_bias)
        )
    )


def body(embeddings, *rest):
    share = embeddings.shape[1] // lax.axis_size("emb")
    dp_size = lax.axis_size("dp")
    whole_tiles = share % 8 == 0 and lax.axis_size("emb") % 4 == 0 and dp_size > 1 and dp_size & (dp_size - 1) == 0
    return (tile_body if whole_tiles else sample_body)(embeddings, *rest)


def solution(mesh):
    return jax.shard_map(
        body,
        mesh=mesh,
        in_specs=(P("emb", "dp", None), P(), P("dp", None), P(), P("emb", None), P("emb", None)),
        out_specs=P("emb", "dp", None),
        check_vma=False,
    )
```

```python
import functools

import jax
import jax.numpy as jnp
from jax import lax
from jax.experimental import pallas as pl
from jax.experimental.pallas import tpu as pltpu
from jax.sharding import PartitionSpec as P

MESH = pl.DeviceIdType.MESH
LANES = 128
VMEM_LIMIT = 40 * 1024 * 1024


def sample_kernel(
    emb_size, dp_size, group, eps,
    x_ref, w_ref, proj_ref, fmb_ref, y_ref,
    got, done, mixed_ref, weights,
    w_send, w_recv, in_send, in_recv, out_send, out_recv, local_sem,
):
    me = lax.axis_index("emb")
    mine = lax.axis_index("dp")
    share = got.shape[0]
    rows = x_ref.shape[1]
    w_rows = w_ref.shape[0]
    entries = float(got.shape[1] * got.shape[2])
    emb_offsets = list(range(1, emb_size))
    dp_offsets = list(range(1, dp_size))

    barrier = pltpu.get_barrier_semaphore()
    for k in emb_offsets:
        pl.semaphore_signal(
            barrier, inc=1, device_id={"emb": lax.rem(me + k, emb_size)}, device_id_type=MESH
        )
    for k in dp_offsets:
        pl.semaphore_signal(
            barrier, inc=1, device_id={"dp": lax.rem(mine + k, dp_size)}, device_id_type=MESH
        )
    pl.semaphore_wait(barrier, len(emb_offsets) + len(dp_offsets))

    def w_copy(k):
        return pltpu.make_async_remote_copy(
            src_ref=w_ref,
            dst_ref=weights.at[pl.ds(pl.multiple_of(mine * w_rows, w_rows), w_rows)],
            send_sem=w_send.at[k],
            recv_sem=w_recv.at[k],
            device_id={"dp": lax.rem(mine + k, dp_size)},
            device_id_type=MESH,
        )

    def in_copy(c, k):
        peer = lax.rem(me + k, emb_size)
        return pltpu.make_async_remote_copy(
            src_ref=x_ref.at[pl.ds(peer * share + c * group, group)],
            dst_ref=got.at[pl.ds(c * group, group), pl.ds(pl.multiple_of(me * rows, rows), rows)],
            send_sem=in_send.at[c, k],
            recv_sem=in_recv.at[c, k],
            device_id={"emb": peer},
            device_id_type=MESH,
        )

    def out_copy(c, k):
        peer = lax.rem(me + k, emb_size)
        return pltpu.make_async_remote_copy(
            src_ref=done.at[pl.ds(c * group, group), pl.ds(pl.multiple_of(peer * rows, rows), rows)],
            dst_ref=y_ref.at[pl.ds(me * share + c * group, group)],
            send_sem=out_send.at[c, k],
            recv_sem=out_recv.at[c, k],
            device_id={"emb": peer},
            device_id_type=MESH,
        )

    def own_in(c):
        return pltpu.make_async_copy(
            x_ref.at[pl.ds(me * share + c * group, group)],
            got.at[pl.ds(c * group, group), pl.ds(pl.multiple_of(me * rows, rows), rows)],
            in_recv.at[c, 0],
        )

    def own_out(c):
        return pltpu.make_async_copy(
            done.at[pl.ds(c * group, group), pl.ds(pl.multiple_of(me * rows, rows), rows)],
            y_ref.at[pl.ds(me * share + c * group, group)],
            out_recv.at[c, 0],
        )

    own_w = pltpu.make_async_copy(
        w_ref, weights.at[pl.ds(pl.multiple_of(mine * w_rows, w_rows), w_rows)], local_sem
    )
    own_w.start()
    for k in dp_offsets:
        w_copy(k).start()

    @pl.loop(0, share // group)
    def _(c):
        for k in emb_offsets:
            in_copy(c, k).start()
        own_in(c).start()

    own_w.wait()
    for k in dp_offsets:
        w_copy(k).wait()

    @pl.loop(0, share // group)
    def _(c):
        own_in(c).wait()
        for k in emb_offsets:
            in_copy(c, k).wait_recv()

        @pl.loop(c * group, (c + 1) * group)
        def _(b):
            x = got[b]
            factor = jnp.dot(proj_ref[...], x, preferred_element_type=jnp.float32).astype(jnp.bfloat16)
            inner = lax.dot_general(
                x, factor, (((1,), (1,)), ((), ())), preferred_element_type=jnp.float32
            ).astype(jnp.bfloat16)
            mixed_ref[...] = (
                jnp.dot(weights[...], x, preferred_element_type=jnp.float32)
                + jnp.dot(inner, fmb_ref[...], preferred_element_type=jnp.float32)
                + x.astype(jnp.float32)
            )
            mixed = mixed_ref[...]
            average = jnp.sum(mixed) / entries
            centered = mixed - average
            spread = jnp.sum(centered * centered) / entries
            scale = lax.rsqrt(jnp.full((1, x.shape[1]), spread + eps, jnp.float32))
            done[b] = (centered * scale).astype(jnp.bfloat16)

        for k in emb_offsets:
            out_copy(c, k).start()
        own_out(c).start()

    @pl.loop(0, share // group)
    def _(c):
        own_out(c).wait()
        for k in emb_offsets:
            in_copy(c, k).wait_send()
            out_copy(c, k).wait()


def sample_body(embeddings, machine_projection, w_lcb, w_fmb, ln_gain, ln_bias):
    emb_size = lax.axis_size("emb")
    dp_size = lax.axis_size("dp")
    rows, samples, width = embeddings.shape
    share = samples // emb_size
    emb_count = w_lcb.shape[1]
    group = 4 if share % 8 == 0 else 2 if share % 2 == 0 else 1
    x = embeddings.transpose(1, 0, 2)
    vmem = pl.BlockSpec(memory_space=pltpu.VMEM)
    y = pl.pallas_call(
        functools.partial(sample_kernel, emb_size, dp_size, group, 1e-05),
        out_shape=jax.ShapeDtypeStruct((samples, rows, width), jnp.bfloat16),
        in_specs=[vmem] * 4,
        out_specs=vmem,
        scratch_shapes=[
            pltpu.VMEM((share, emb_count, width), jnp.bfloat16),
            pltpu.VMEM((share, emb_count, width), jnp.bfloat16),
            pltpu.VMEM((emb_count, width), jnp.float32),
            pltpu.VMEM((emb_count, emb_count), jnp.bfloat16),
            pltpu.SemaphoreType.DMA((dp_size,)),
            pltpu.SemaphoreType.DMA((dp_size,)),
            pltpu.SemaphoreType.DMA((share // group, emb_size)),
            pltpu.SemaphoreType.DMA((share // group, emb_size)),
            pltpu.SemaphoreType.DMA((share // group, emb_size)),
            pltpu.SemaphoreType.DMA((share // group, emb_size)),
            pltpu.SemaphoreType.DMA(()),
        ],
        compiler_params=pltpu.CompilerParams(
            collective_id=0, has_side_effects=True, vmem_limit_bytes=40 * 1024 * 1024
        ),
    )(x, w_lcb, machine_projection.T, w_fmb)
    scaled = y.transpose(1, 0, 2).astype(jnp.float32)
    return (scaled * ln_gain[:, None, :] + ln_bias[:, None, :]).astype(jnp.bfloat16)


def tile_kernel(
    emb_size, dp_size, cores, eps,
    x_hbm, w_hbm, proj_hbm, fmb_hbm, gain_hbm, bias_hbm, y_ref,
    own, got, done, back, wide, spaced, mixed_ref, weights, factors, affine,
    w_send, w_recv, send_sem, in_recv, out_recv, load_sem, outer, beside, far,
):
    me = lax.axis_index("emb")
    mine = lax.axis_index("dp")
    chips = emb_size // cores
    chip = me // cores
    emb_count, share, width = got.shape
    rows = x_hbm.shape[0]
    w_rows = w_hbm.shape[0]
    block = rows * share
    others = emb_size - 1
    entries = float(emb_count * width)
    columns = [pl.ds(c, LANES) for c in range(0, width, LANES)]
    near = [sign * step for step in range(1, chips) for sign in (1, -1)]
    half = max(chips // 2, 1)
    dp_bits = [1 << i for i in range(dp_size.bit_length() - 1)]

    def inside(other):
        return (other >= 0) & (other < chips)

    def on_chip(step, action):
        other = chip + step

        @pl.when(inside(other))
        def _():
            for k in range(cores):
                peer = other * cores + k
                if step:
                    action(peer)
                else:
                    pl.when(peer != me)(functools.partial(action, peer))

    def same_side_then_across(action):
        for crossing in (False, True):
            for step in reversed(near) if crossing else near:
                other = chip + step
                across = (other // half) != (chip // half)

                @pl.when(inside(other) & (across if crossing else jnp.logical_not(across)))
                def _():
                    for k in range(cores):
                        action(other * cores + k)
            if not crossing:
                on_chip(0, action)

    def dp_partner(bit):
        return mine + bit * (1 - 2 * lax.rem(mine // bit, 2))

    def of_peer(ref, peer):
        return ref.at[:, pl.ds(pl.multiple_of(peer * share, share), share)]

    def signal(semaphore, peer):
        pl.semaphore_signal(semaphore, inc=1, device_id={"emb": peer}, device_id_type=MESH)

    inward = 1 - 2 * (chip // half if chips > 1 else chip)
    inward = jnp.maximum(inward, -1)
    middle = (chip == half - 1) | (chip == half)
    core = lax.rem(me, cores)
    neighbours = (me + inward * cores, me - inward * cores)
    there = (inside(chip + inward), inside(chip - inward))

    barrier = pltpu.get_barrier_semaphore()
    pl.when(there[0] & middle)(functools.partial(signal, barrier, neighbours[0]))
    pl.when(there[1])(functools.partial(signal, barrier, neighbours[1]))

    @pl.when(core == 0)
    def _():
        for bit in dp_bits:
            pl.semaphore_signal(barrier, inc=1, device_id={"dp": dp_partner(bit)}, device_id_type=MESH)

    @pl.when(core != 0)
    def _():
        signal(barrier, me - core)

    own_in = pltpu.make_async_copy(of_peer(x_hbm, me), own, load_sem.at[0])
    own_w = pltpu.make_async_copy(
        w_hbm, weights.at[pl.ds(pl.multiple_of(mine * w_rows, w_rows), w_rows)], load_sem.at[1]
    )

    def in_copy(source, peer):
        return pltpu.make_async_remote_copy(
            src_ref=of_peer(x_hbm, peer),
            dst_ref=got.at[pl.ds(source * rows, rows)],
            send_sem=send_sem,
            recv_sem=in_recv,
            device_id={"emb": peer},
            device_id_type=MESH,
        )

    def last_source(receiver):
        return jnp.where(receiver // cores < half, half, half - 1) * cores + cores - 1

    tail = max(rows // 16, 1)
    parts = ((0, rows - tail), (rows - tail, tail))

    def out_copy(source, peer, start=0, size=rows, slot=0):
        return pltpu.make_async_remote_copy(
            src_ref=done.at[pl.ds(peer * rows + start, size)],
            dst_ref=back.at[source, pl.ds(start, size)],
            send_sem=send_sem,
            recv_sem=out_recv.at[slot],
            device_id={"emb": peer},
            device_id_type=MESH,
        )

    def send_back(peer):
        ends = me == last_source(peer)
        pl.when(jnp.logical_not(ends))(lambda: out_copy(me, peer).start())

        @pl.when(ends)
        def _():
            for slot, (start, size) in enumerate(parts, 1):
                out_copy(me, peer, start, size, slot).start()

    def w_copy(i):
        bit = dp_bits[i]
        held = pl.multiple_of((mine // bit) * (bit * w_rows), bit * w_rows)
        part = weights.at[pl.ds(held, bit * w_rows)]
        return pltpu.make_async_remote_copy(
            src_ref=part,
            dst_ref=part,
            send_sem=w_send,
            recv_sem=w_recv.at[i],
            device_id={"dp": dp_partner(bit)},
            device_id_type=MESH,
        )

    def w_pass(peer):
        return pltpu.make_async_remote_copy(
            src_ref=weights,
            dst_ref=weights,
            send_sem=w_send,
            recv_sem=w_recv.at[0],
            device_id={"emb": peer},
            device_id_type=MESH,
        )

    def wait_for(ref, semaphore):
        pltpu.make_async_copy(ref, ref, semaphore).wait()

    def tell(distance):
        for sign in (1, -1):
            @pl.when(inside(chip + sign * (distance - 1)) & inside(chip - sign))
            def _():
                signal(far.at[distance - 2], me - sign * cores)

    def heard(distance):
        count = inside(chip + distance).astype(jnp.int32) + inside(chip - distance).astype(jnp.int32)

        @pl.when(count > 0)
        def _():
            pl.semaphore_wait(far.at[distance - 2], count)

    pl.semaphore_wait(
        barrier,
        there[0].astype(jnp.int32) + jnp.where(core == 0, cores - 1 + len(dp_bits), 0),
    )
    pl.when(there[0])(lambda: in_copy(me, neighbours[0]).start())
    own_in.start()
    pl.when(there[0] & jnp.logical_not(middle))(functools.partial(signal, outer, neighbours[0]))

    @pl.when(there[1])
    def _():
        pl.semaphore_wait(outer, 1)
        in_copy(me, neighbours[1]).start()

    @pl.when(core == 0)
    def _():
        own_w.start()
        for k in range(1, cores):
            signal(beside, me + k)
        if cores > 1:
            pl.semaphore_wait(beside, cores - 1)

    @pl.when(core != 0)
    def _():
        pl.semaphore_wait(beside, 1)
        signal(beside, me - core)

    for source, first in ((proj_hbm, 0), (fmb_hbm, emb_count)):
        target = factors.at[:, pl.ds(first, source.shape[1])]
        pltpu.make_async_copy(source, target, load_sem.at[0]).start()
    for i, source in enumerate((gain_hbm, bias_hbm)):
        pltpu.make_async_copy(source, affine.at[i], load_sem.at[0]).start()
    if chips > 2:
        tell(2)

    for k in range(cores):
        for distance in range(chips):
            if k == 0 and distance >= 2:
                heard(distance)
                if distance < chips - 1:
                    tell(distance + 1)
            for step in (distance, -distance) if distance else (0,):
                peer = (chip + step) * cores + k
                left = peer != me + step * cores if distance < 2 else True

                @pl.when(inside(chip + step) & left)
                def _():
                    in_copy(me, peer).start()

    @pl.when(core == 0)
    def _():
        own_w.wait()
        for i in range(len(dp_bits)):
            w_copy(i).start()
            w_copy(i).wait_recv()
        for k in range(1, cores):
            w_pass(me + k).start()

    @pl.when(core != 0)
    def _():
        w_pass(me - core).wait_recv()

    loaded = 2 * (own.size + factors.size) + 4 * affine.size
    wait_for(wide.at[0, pl.ds(0, loaded // (4 * LANES))], load_sem.at[0])

    def widen(source, taken):
        taken = taken.astype(jnp.float32).reshape(block, width)
        for c in range(len(columns)):
            wide[c, pl.ds(pl.multiple_of(source * block, block), block)] = taken[:, c * LANES:(c + 1) * LANES]

    widen(me, own[...])
    wait_for(got.at[pl.ds(0, others * rows)], in_recv)

    @pl.loop(0, emb_size)
    def _(source):
        @pl.when(source != me)
        def _():
            widen(source, got[pl.ds(source * rows, rows)])

    @pl.loop(0, share)
    def _(b):
        x = jnp.concatenate(
            [wide[c, pl.ds(b, emb_count, stride=share), :] for c in range(len(columns))], axis=1
        ).astype(jnp.bfloat16)
        factor = jnp.dot(
            factors[:, :emb_count], x, preferred_element_type=jnp.float32
        ).astype(jnp.bfloat16)
        inner = lax.dot_general(
            x, factor, (((1,), (1,)), ((), ())), preferred_element_type=jnp.float32
        ).astype(jnp.bfloat16)
        mixed_ref[...] = (
            jnp.dot(weights[...], x, preferred_element_type=jnp.float32)
            + jnp.dot(inner, factors[:, emb_count:], preferred_element_type=jnp.float32)
            + x.astype(jnp.float32)
        )
        mixed = mixed_ref[...]
        average = jnp.sum(mixed) / entries
        centered = mixed - average
        spread = jnp.sum(centered * centered) / entries
        scale = lax.rsqrt(jnp.full((1, width), spread + eps, jnp.float32))
        scaled = centered * scale
        for c in range(len(columns)):
            spaced[c, pl.ds(b, emb_count, stride=share), :] = scaled[:, c * LANES:(c + 1) * LANES]

    def narrow(target):
        for c, column in enumerate(columns):
            done[pl.ds(target * rows, rows), :, column] = (
                spaced[c, pl.ds(pl.multiple_of(target * block, block), block)]
                .reshape(rows, share, LANES)
                .astype(jnp.bfloat16)
            )

    def land(source, taken, start=0):
        part = pl.ds(start, taken.shape[0])
        y_ref[part, pl.ds(pl.multiple_of(source * share, share), share), :] = (
            taken.astype(jnp.float32) * affine[0, part][:, None, :] + affine[1, part][:, None, :]
        ).astype(jnp.bfloat16)

    pl.loop(0, emb_size)(narrow)
    land(me, done[pl.ds(me * rows, rows)])
    same_side_then_across(send_back)

    @pl.when(core == 0)
    def _():
        wait_for(weights.at[pl.ds(0, (dp_size - 1) * w_rows)], w_send)
        for k in range(1, cores):
            w_pass(me + k).wait_send()

    last = last_source(me)
    wait_for(back.at[pl.ds(0, others - 1)], out_recv.at[0])

    @pl.loop(0, emb_size)
    def _(source):
        @pl.when((source != me) & (source != last))
        def _():
            land(source, back[source])

    for slot, (start, size) in enumerate(parts, 1):
        wait_for(back.at[0, pl.ds(start, size)], out_recv.at[slot])
        land(last, back[last, pl.ds(start, size)], start)
    wait_for(wide.at[:, pl.ds(0, others * block)], send_sem)


def tile_body(embeddings, machine_projection, w_lcb, w_fmb, ln_gain, ln_bias):
    emb_size = lax.axis_size("emb")
    dp_size = lax.axis_size("dp")
    rows, samples, width = embeddings.shape
    share = samples // emb_size
    emb_count, rank = machine_projection.shape
    cores = 2 if emb_size % 2 == 0 else 1
    dma = pltpu.SemaphoreType.DMA
    return pl.pallas_call(
        functools.partial(tile_kernel, emb_size, dp_size, cores, 1e-05),
        out_shape=pltpu.VMEM((rows, samples, width), jnp.bfloat16),
        in_specs=[pl.BlockSpec(memory_space=pltpu.HBM)] * 6,
        out_specs=pl.BlockSpec(memory_space=pltpu.VMEM),
        scratch_shapes=[
            pltpu.VMEM((rows, share, width), jnp.bfloat16),
            pltpu.VMEM((emb_count, share, width), jnp.bfloat16),
            pltpu.VMEM((emb_count, share, width), jnp.bfloat16),
            pltpu.VMEM((emb_size, rows, share, width), jnp.bfloat16),
            pltpu.VMEM((width // LANES, emb_count * share, LANES), jnp.float32),
            pltpu.VMEM((width // LANES, emb_count * share, LANES), jnp.float32),
            pltpu.VMEM((emb_count, width), jnp.float32),
            pltpu.VMEM((emb_count, emb_count), jnp.bfloat16),
            pltpu.VMEM((rank, emb_count + width), jnp.bfloat16),
            pltpu.VMEM((2, rows, width), jnp.float32),
            dma(()),
            dma((dp_size.bit_length() - 1,)),
            dma(()),
            dma(()),
            dma((3,)),
            dma((2,)),
            pltpu.SemaphoreType.REGULAR,
            pltpu.SemaphoreType.REGULAR,
            pltpu.SemaphoreType.REGULAR((max(emb_size // cores - 2, 1),)),
        ],
        compiler_params=pltpu.CompilerParams(
            collective_id=0, has_side_effects=True, vmem_limit_bytes=VMEM_LIMIT
        ),
    )(
        *(
            pltpu.with_memory_space_constraint(array, pltpu.HBM)
            for array in (embeddings, w_lcb, machine_projection.T, w_fmb, ln_gain, ln_bias)
        )
    )


def body(embeddings, *rest):
    share = embeddings.shape[1] // lax.axis_size("emb")
    dp_size = lax.axis_size("dp")
    whole_tiles = share % 8 == 0 and lax.axis_size("emb") % 4 == 0 and dp_size > 1 and dp_size & (dp_size - 1) == 0
    return (tile_body if whole_tiles else sample_body)(embeddings, *rest)


def solution(mesh):
    return jax.shard_map(
        body,
        mesh=mesh,
        in_specs=(P("emb", "dp", None), P(), P("dp", None), P(), P("emb", None), P("emb", None)),
        out_specs=P("emb", "dp", None),
        check_vma=False,
    )
```
